8 devices in a mesh: rep: 1 (over z), dp: 2 (over y), sp: 4 (over x, core).
Axes of the slice: x: 2, y: 2, z: 1, core: 2. Of those that a mesh axis runs over, the one named last changes fastest.
Arguments:
- hidden: bfloat16 [128, 2048], P(('rep', 'dp'))
- w_query: bfloat16 [2048, 2048], replicated
- w_key: bfloat16 [2048, 256], replicated
- w_value: bfloat16 [2048, 256], replicated
- w_out: bfloat16 [2048, 2048], P('sp')
- k_cache: bfloat16 [128, 2048, 1, 256], P(('rep', 'dp'), 'sp')
- v_cache: bfloat16 [128, 2048, 1, 256], P(('rep', 'dp'), 'sp')
- write_pos: int32 [128], P(('rep', 'dp'))
- valid_len: int32 [128], P(('rep', 'dp'))
Outputs:
- output 1: bfloat16 [128, 2048], P(('rep', 'dp'))
- output 2: bfloat16 [128, 2048, 1, 256], P(('rep', 'dp'), 'sp')
- output 3: bfloat16 [128, 2048, 1, 256], P(('rep', 'dp'), 'sp')
All inputs are finite; a program needn't handle non-finite values.
Results may differ from the reference program's by a relative error of at most 0.00615348.
Values are sent between devices in bfloat16 or wider.
A program may use at most 1 GiB of HBM per device.

```python
import jax
import jax.numpy as jnp
from jax import lax

MODEL_DIM = 2048
NUM_HEADS = 8
KV_HEADS = 1
HEAD_DIM = 256
BATCH_SIZE = 128
CACHE_LEN = 2048
SEGMENTS = 16


def draw_lengths(rng_key):
    keys = jax.random.split(rng_key, 3)
    shortest = CACHE_LEN // 4
    write_pos = jax.random.randint(keys[0], (BATCH_SIZE,), shortest - 1, CACHE_LEN, jnp.int32)
    long_row = jax.random.randint(keys[1], (), 0, BATCH_SIZE, jnp.int32)
    short_row = (long_row + 1 + jax.random.randint(keys[2], (), 0, BATCH_SIZE - 1, jnp.int32)) % BATCH_SIZE
    row_ids = jnp.arange(BATCH_SIZE, dtype=jnp.int32)
    write_pos = jnp.where(row_ids == long_row, CACHE_LEN - 1, write_pos)
    write_pos = jnp.where(row_ids == short_row, shortest - 1, write_pos)
    return write_pos, write_pos + 1


def setup_inputs(seed: int = 0, part: int = 0) -> dict:
    root = jax.random.key(seed)
    shared = jax.random.split(root, 4)
    own = jax.random.split(jax.random.fold_in(root, part), 8)
    seg_len = CACHE_LEN // SEGMENTS
    proj_width = NUM_HEADS * HEAD_DIM
    kv_width = KV_HEADS * HEAD_DIM
    w_query = (jax.random.normal(shared[0], (MODEL_DIM, proj_width), jnp.float32) * MODEL_DIM ** -0.5).astype(jnp.bfloat16)
    w_key = (jax.random.normal(shared[1], (MODEL_DIM, kv_width), jnp.float32) * MODEL_DIM ** -0.5).astype(jnp.bfloat16)
    w_value = (jax.random.normal(shared[2], (MODEL_DIM, kv_width), jnp.float32) * MODEL_DIM ** -0.5).astype(jnp.bfloat16)
    w_out = (jax.random.normal(shared[3], (proj_width, MODEL_DIM), jnp.float32) * proj_width ** -0.5).astype(jnp.bfloat16)
    hidden = jax.random.normal(own[0], (BATCH_SIZE, MODEL_DIM), jnp.float32).astype(jnp.bfloat16)
    cache_shape = (BATCH_SIZE, SEGMENTS, seg_len, KV_HEADS, HEAD_DIM)
    seg_shape = (BATCH_SIZE, SEGMENTS, 1, KV_HEADS, HEAD_DIM)
    flat_shape = (BATCH_SIZE, CACHE_LEN, KV_HEADS, HEAD_DIM)
    k_cache = (jax.random.normal(own[1], cache_shape, jnp.float32) + jax.random.normal(own[2], seg_shape, jnp.float32)).reshape(flat_shape).astype(jnp.bfloat16)
    v_cache = (jax.random.normal(own[3], cache_shape, jnp.float32) + jax.random.normal(own[4], seg_shape, jnp.float32)).reshape(flat_shape).astype(jnp.bfloat16)
    write_pos, valid_len = draw_lengths(own[5])
    return {'hidden': hidden, 'w_query': w_query, 'w_key': w_key, 'w_value': w_value, 'w_out': w_out, 'k_cache': k_cache, 'v_cache': v_cache, 'write_pos': write_pos, 'valid_len': valid_len}


def reference(hidden, w_query, w_key, w_value, w_out, k_cache, v_cache, write_pos, valid_len):
    group_size = NUM_HEADS // KV_HEADS
    query = jnp.dot(hidden, w_query, preferred_element_type=jnp.float32).astype(jnp.bfloat16)
    query = query.reshape(BATCH_SIZE, KV_HEADS, group_size, HEAD_DIM)
    key_new = jnp.dot(hidden, w_key, preferred_element_type=jnp.float32).astype(jnp.bfloat16)
    value_new = jnp.dot(hidden, w_value, preferred_element_type=jnp.float32).astype(jnp.bfloat16)
    positions = jnp.arange(CACHE_LEN, dtype=jnp.int32)
    at_pos = (positions[None, :] == write_pos[:, None])[:, :, None, None]
    k_next = jnp.where(at_pos, key_new.reshape(BATCH_SIZE, 1, KV_HEADS, HEAD_DIM), k_cache)
    v_next = jnp.where(at_pos, value_new.reshape(BATCH_SIZE, 1, KV_HEADS, HEAD_DIM), v_cache)

    def one_row(row_args):
        q_row, k_row, v_row, length = row_args
        scores = jnp.einsum('kgd,skd->kgs', q_row.astype(jnp.float32), k_row.astype(jnp.float32)) * HEAD_DIM ** -0.5
        scores = jnp.where(positions < length, scores, -jnp.inf)
        row_max = jnp.max(scores, axis=-1, keepdims=True)
        weights = jnp.exp(scores - row_max)
        total = jnp.sum(weights, axis=-1, keepdims=True)
        return jnp.einsum('kgs,skd->kgd', weights, v_row.astype(jnp.float32)) / total

    attention = lax.map(one_row, (query, k_next, v_next, valid_len))
    attention = attention.reshape(BATCH_SIZE, NUM_HEADS * HEAD_DIM).astype(jnp.bfloat16)
    attn_out = jnp.dot(attention, w_out, preferred_element_type=jnp.float32).astype(jnp.bfloat16)
    return (attn_out, k_next, v_next)
```

```python
import functools

import jax
import jax.numpy as jnp
from jax import lax
from jax.experimental import pallas as pl
from jax.experimental.pallas import tpu as pltpu
from jax.sharding import PartitionSpec as P

F32, BF16 = jnp.float32, jnp.bfloat16
NEG_FLOOR = -1e30
GROUP = 8
AHEAD = 3
ANY = pl.BlockSpec(memory_space=pl.ANY)
VMEM = pl.BlockSpec(memory_space=pltpu.VMEM)


def attend(hid_hbm, wq_hbm, wk_hbm, wv_hbm, k_hbm, v_hbm, pos_hbm, len_hbm,
           acc_ref, ml_ref, k_out, v_out,
           hid, wq, wk, wv, q_all, k_row, v_row, pos, length, sem_w, sem_s, sem_k, sem_v):
    rows, span, dim = k_out.shape
    heads = q_all.shape[0]
    groups = rows // GROUP
    start = lax.axis_index('sp') * span

    def fetch(g):
        part = pl.ds(g * GROUP, GROUP)
        return (pltpu.make_async_copy(k_hbm.at[part], k_out.at[part], sem_k.at[g]),
                pltpu.make_async_copy(v_hbm.at[part], v_out.at[part], sem_v.at[g]))

    def q_part(h):
        cols = pl.ds(h * dim, dim)
        return pltpu.make_async_copy(wq_hbm.at[:, cols], wq.at[:, cols], sem_w.at[3 + h])

    scal = [pltpu.make_async_copy(pos_hbm, pos, sem_s.at[0]), pltpu.make_async_copy(len_hbm, length, sem_s.at[1])]
    first = [pltpu.make_async_copy(hid_hbm, hid, sem_w.at[0]),
             pltpu.make_async_copy(wk_hbm, wk, sem_w.at[1]),
             pltpu.make_async_copy(wv_hbm, wv, sem_w.at[2])]
    for c in scal + first + [q_part(h) for h in range(heads)]:
        c.start()
    for g in range(AHEAD):
        for c in fetch(g):
            c.start()
    for c in scal:
        c.wait()
    first[0].wait()
    first[1].wait()
    k_row[...] = jnp.dot(hid[...], wk[...], preferred_element_type=F32).astype(BF16).astype(F32)
    first[2].wait()
    v_row[...] = jnp.dot(hid[...], wv[...], preferred_element_type=F32).astype(BF16).astype(F32)
    for h in range(heads):
        q_part(h).wait()
        q_all[h] = jnp.dot(hid[...], wq[:, h * dim:(h + 1) * dim], preferred_element_type=F32).astype(BF16).astype(F32)

    def step(g, ml):
        for c in fetch(g):
            c.wait()

        @pl.when(g + AHEAD < groups)
        def _():
            for c in fetch(g + AHEAD):
                c.start()

        base = g * GROUP
        q = jnp.swapaxes(q_all[:, pl.ds(pl.multiple_of(base, GROUP), GROUP), :], 0, 1)
        sub = lax.broadcasted_iota(jnp.int32, (16, dim), 0)
        for j in range(GROUP):
            at = pos[base + j] - start
            inside = jnp.logical_and(at >= 0, at < span)
            at = jnp.where(inside, at, 0)
            win = pl.ds(pl.multiple_of(at // 16 * 16, 16), 16)
            hit = jnp.logical_and(sub == at % 16, inside)
            for row, buf in ((k_row, k_out), (v_row, v_out)):
                new = row[pl.ds(base + j, 1), :]
                old = buf[base + j, win, :].astype(F32)
                buf[base + j, win, :] = jnp.where(hit, new, old).astype(BF16)
        col = lax.broadcasted_iota(jnp.int32, (heads, span), 1)
        lane = lax.broadcasted_iota(jnp.int32, ml.shape, 1)
        scores = []
        for j in range(GROUP):
            s = lax.dot_general(q[j].astype(BF16), k_out[base + j], (((1,), (1,)), ((), ())), preferred_element_type=F32)
            scores.append(jnp.where(col < length[base + j] - start, s * dim ** -0.5, -jnp.inf))
        probs = []
        for j in range(GROUP):
            m = jnp.maximum(jnp.max(scores[j], axis=1, keepdims=True), NEG_FLOOR)
            p = jnp.exp(scores[j] - m)
            ml = jnp.where(lane == base + j, m, ml)
            ml = jnp.where(lane == rows + base + j, jnp.sum(p, axis=1, keepdims=True), ml)
            probs.append(p.astype(BF16))
        out = [jnp.dot(probs[j], v_out[base + j], preferred_element_type=F32) for j in range(GROUP)]
        acc_ref[:, pl.ds(pl.multiple_of(base, GROUP), GROUP), :] = jnp.swapaxes(jnp.stack(out), 0, 1)
        return ml

    ml_ref[...] = lax.fori_loop(0, groups, step, jnp.zeros(ml_ref.shape, F32))


def finish(acc, ml, wo_hbm, out, wo, ml_in, part1, send2, part2, mine, half, part3, send4, part4, done, part5,
           sem_w, send, recv):
    i = lax.axis_index('sp')
    x, c = i // 2, i % 2
    pair, across, far = 2 * x + 1 - c, 2 * (1 - x) + c, 2 * (1 - x) + 1 - c
    rows = acc.shape[1]
    wide = half.shape[2]
    barrier = pltpu.get_barrier_semaphore()
    for peer in (pair, across, far):
        pl.semaphore_signal(barrier, inc=1, device_id={'sp': peer}, device_id_type=pl.DeviceIdType.MESH)
    load = pltpu.make_async_copy(wo_hbm, wo, sem_w)
    load.start()
    pl.semaphore_wait(barrier, 3)

    def to(n, src, dst, peer):
        return pltpu.make_async_remote_copy(src_ref=src, dst_ref=dst, send_sem=send.at[n], recv_sem=recv.at[n],
                                            device_id={'sp': peer}, device_id_type=pl.DeviceIdType.MESH)

    def heads_of(xx, cc):
        return 4 * xx + 2 * cc

    c_ml = [to(n, ml, ml_in.at[n], peer) for n, peer in enumerate((pair, across, far))]
    c_1 = [to(3, acc.at[pl.ds(heads_of(1 - x, 1 - c), 2)], part1.at[0], pair),
           to(4, acc.at[pl.ds(heads_of(x, 1 - c), 2)], part1.at[1], pair)]
    for copy in c_ml + c_1:
        copy.start()

    def split(v):
        t = v.T
        return t[:rows], t[rows:]

    lane = lax.broadcasted_iota(jnp.int32, (rows, ml.shape[0]), 1)

    def col(v, h):
        return jnp.sum(jnp.where(lane == h, v, 0.0), axis=1, keepdims=True)

    m0, l0 = split(ml[...])
    c_ml[0].wait()
    m1, l1 = split(ml_in[0])
    mp = jnp.maximum(m0, m1)
    e0, e1 = jnp.exp(m0 - mp), jnp.exp(m1 - mp)
    lp = l0 * e0 + l1 * e1
    c_1[0].wait()
    for j in range(2):
        h = heads_of(1 - x, c) + j
        send2[j] = acc[h] * col(e0, h) + part1[0, j] * col(e1, h)
    c_2 = to(5, send2, part2, across)
    c_2.start()
    c_1[1].wait()
    for j in range(2):
        h = heads_of(x, c) + j
        mine[j] = acc[h] * col(e0, h) + part1[1, j] * col(e1, h)
    c_ml[1].wait()
    c_ml[2].wait()
    m2, l2 = split(ml_in[1])
    m3, l3 = split(ml_in[2])
    mq = jnp.maximum(m2, m3)
    lq = l2 * jnp.exp(m2 - mq) + l3 * jnp.exp(m3 - mq)
    mt = jnp.maximum(mp, mq)
    ep, eq = jnp.exp(mp - mt), jnp.exp(mq - mt)
    inv = 1.0 / (lp * ep + lq * eq)
    ep, eq = ep * inv, eq * inv
    factors = [(col(ep, heads_of(x, c) + j), col(eq, heads_of(x, c) + j)) for j in range(2)]
    load.wait()
    c_2.wait()
    o = jnp.concatenate([(mine[j] * factors[j][0] + part2[j] * factors[j][1]).astype(BF16) for j in range(2)], axis=1)

    def project(side):
        cols = pl.ds(pl.multiple_of(side * wide, wide), wide)
        return jnp.dot(o, wo[:, cols], preferred_element_type=F32)

    half[0] = project(1 - c)
    c_3 = to(6, half.at[0], part3, pair)
    c_3.start()
    half[1] = project(c)
    c_3.wait()
    send4[...] = half[1] + part3[...]
    c_4 = to(7, send4, part4, across)
    c_4.start()
    c_4.wait()
    done[...] = (send4[...] + part4[...]).astype(BF16)
    c_5 = to(8, done, part5, pair)
    c_5.start()
    out[:, pl.ds(pl.multiple_of(c * wide, wide), wide)] = done[...]
    c_5.wait()
    out[:, pl.ds(pl.multiple_of((1 - c) * wide, wide), wide)] = part5[...]


def solution(mesh):
    row_spec = P(('rep', 'dp'), None)
    cache_spec = P(('rep', 'dp'), 'sp', None, None)
    len_spec = P(('rep', 'dp'))

    def local_step(hidden, w_query, w_key, w_value, w_out, k_cache, v_cache, write_pos, valid_len):
        rows, span, kv_heads, dim = k_cache.shape
        model = hidden.shape[1]
        heads = w_query.shape[1] // dim
        cache = (rows, span, dim)
        hbm = lambda a: pltpu.with_memory_space_constraint(a, pltpu.HBM)
        acc, ml, k_new, v_new = pl.pallas_call(
            attend,
            out_shape=[jax.ShapeDtypeStruct((heads, rows, dim), F32),
                       jax.ShapeDtypeStruct((heads, 2 * rows), F32),
                       pltpu.VMEM(cache, BF16), pltpu.VMEM(cache, BF16)],
            in_specs=[ANY] * 8,
            out_specs=[VMEM, VMEM, VMEM, VMEM],
            scratch_shapes=[pltpu.VMEM((rows, model), BF16), pltpu.VMEM(w_query.shape, BF16),
                            pltpu.VMEM(w_key.shape, BF16), pltpu.VMEM(w_value.shape, BF16),
                            pltpu.VMEM((heads, rows, dim), F32), pltpu.VMEM((rows, dim), F32), pltpu.VMEM((rows, dim), F32),
                            pltpu.SMEM((rows,), jnp.int32), pltpu.SMEM((rows,), jnp.int32),
                            pltpu.SemaphoreType.DMA((3 + heads,)), pltpu.SemaphoreType.DMA((2,)),
                            pltpu.SemaphoreType.DMA((rows // GROUP,)), pltpu.SemaphoreType.DMA((rows // GROUP,))],
            compiler_params=pltpu.CompilerParams(vmem_limit_bytes=16 * 2 ** 20),
            cost_estimate=pl.CostEstimate(flops=10 ** 9, bytes_accessed=46 * 10 ** 6, transcendentals=0),
            name='attend',
        )(*map(hbm, (hidden, w_query, w_key, w_value, k_cache.reshape(cache), v_cache.reshape(cache), write_pos, valid_len)))
        wide = w_out.shape[1] // 2
        pair = (2, rows, dim)
        attn_out = pl.pallas_call(
            finish,
            out_shape=jax.ShapeDtypeStruct((rows, w_out.shape[1]), BF16),
            in_specs=[VMEM, VMEM, ANY],
            out_specs=VMEM,
            scratch_shapes=[pltpu.VMEM(w_out.shape, BF16), pltpu.VMEM((3, heads, 2 * rows), F32),
                            pltpu.VMEM((2,) + pair, F32), pltpu.VMEM(pair, F32), pltpu.VMEM(pair, F32), pltpu.VMEM(pair, F32),
                            pltpu.VMEM((2, rows, wide), F32), pltpu.VMEM((rows, wide), F32), pltpu.VMEM((rows, wide), F32),
                            pltpu.VMEM((rows, wide), F32), pltpu.VMEM((rows, wide), BF16), pltpu.VMEM((rows, wide), BF16),
                            pltpu.SemaphoreType.DMA, pltpu.SemaphoreType.DMA((9,)), pltpu.SemaphoreType.DMA((9,))],
            compiler_params=pltpu.CompilerParams(collective_id=0, has_side_effects=True, vmem_limit_bytes=12 * 2 ** 20),
            cost_estimate=pl.CostEstimate(flops=10 ** 9, bytes_accessed=4 * 10 ** 6, transcendentals=0),
            name='finish',
        )(acc, ml, w_out)
        return attn_out, k_new.reshape(k_cache.shape), v_new.reshape(v_cache.shape)

    return jax.shard_map(local_step, mesh=mesh, in_specs=(row_spec, P(), P(), P(), P('sp', None), cache_spec, cache_spec, len_spec, len_spec), out_specs=(row_spec, cache_spec, cache_spec), check_vma=False)
```

```python
import functools

import jax
import jax.numpy as jnp
from jax import lax
from jax.experimental import pallas as pl
from jax.experimental.pallas import tpu as pltpu
from jax.sharding import PartitionSpec as P

F32, BF16 = jnp.float32, jnp.bfloat16
NEG_FLOOR = -1e30
GROUP = 8
AHEAD = 4
CHUNKS = ((0, 32), (32, 48), (48, 64))
PLAN = {3: ((0, 0),), 4: ((1, 0),), 5: ((0, 1),), 6: ((2, 0), (1, 1)), 7: ((0, 2), (3, 0)),
        8: ((1, 2), (2, 1), (4, 0), (2, 2), (3, 1), (3, 2), (5, 0), (4, 1), (4, 2), (5, 1), (5, 2))}
ANY = pl.BlockSpec(memory_space=pl.ANY)
VMEM = pl.BlockSpec(memory_space=pltpu.VMEM)
SMEM = pl.BlockSpec(memory_space=pltpu.SMEM)
MESH = pl.DeviceIdType.MESH


def attend(hid_hbm, wq_hbm, wk_hbm, wv_hbm, wo_hbm, k_hbm, v_hbm, pos_hbm, len_hbm,
           att, k_buf, v_buf, k_row, v_row,
           hid, wq, wk, wv, wo, q_all, pos, length, acc, ml, ml_in, part1, send2, part2, mine, half, part3, send4, part4, done, part5,
           sem_w, sem_s, sem_k, sem_v, send, recv):
    rows, span, dim = k_buf.shape
    heads = q_all.shape[0]
    groups = rows // GROUP
    wide = half.shape[2]
    i = lax.axis_index('sp')
    x, c = i // 2, i % 2
    pair, across, far = 2 * x + 1 - c, 2 * (1 - x) + c, 2 * (1 - x) + 1 - c
    start = i * span
    barrier = pltpu.get_barrier_semaphore()
    for peer in (pair, across, far):
        pl.semaphore_signal(barrier, inc=1, device_id={'sp': peer}, device_id_type=MESH)

    def fetch(g):
        part = pl.ds(g * GROUP, GROUP)
        return (pltpu.make_async_copy(k_hbm.at[part], k_buf.at[part], sem_k.at[g]),
                pltpu.make_async_copy(v_hbm.at[part], v_buf.at[part], sem_v.at[g]))

    def q_part(h):
        cols = pl.ds(h * dim, dim)
        return pltpu.make_async_copy(wq_hbm.at[:, cols], wq.at[:, cols], sem_w.at[4 + h])

    scal = [pltpu.make_async_copy(pos_hbm, pos, sem_s.at[0]), pltpu.make_async_copy(len_hbm, length, sem_s.at[1])]
    first = [pltpu.make_async_copy(hid_hbm, hid, sem_w.at[0]),
             pltpu.make_async_copy(wk_hbm, wk, sem_w.at[1]),
             pltpu.make_async_copy(wv_hbm, wv, sem_w.at[2])]
    last = pltpu.make_async_copy(wo_hbm, wo, sem_w.at[3])
    for copy in scal + first + [q_part(h) for h in range(heads)]:
        copy.start()
    for g in range(AHEAD):
        for copy in fetch(g):
            copy.start()
    for copy in scal:
        copy.wait()
    first[0].wait()
    first[1].wait()
    k_row[...] = jnp.dot(hid[...], wk[...], preferred_element_type=F32).astype(BF16).astype(F32)
    first[2].wait()
    v_row[...] = jnp.dot(hid[...], wv[...], preferred_element_type=F32).astype(BF16).astype(F32)
    for h in range(heads):
        q_part(h).wait()
        q_all[h] = jnp.dot(hid[...], wq[:, h * dim:(h + 1) * dim], preferred_element_type=F32).astype(BF16).astype(F32)

    def group_step(g, k):
        for copy in fetch(g):
            copy.wait()
        if g + AHEAD < groups:
            for copy in fetch(g + AHEAD):
                copy.start()
        if g == 0:
            last.start()
        base = g * GROUP
        here = slice(base, base + GROUP)
        q = jnp.swapaxes(q_all[:, here, :], 0, 1)
        fresh = jnp.sum(q * k_row[here, :][:, None, :], axis=2, keepdims=True) * dim ** -0.5
        col = lax.broadcasted_iota(jnp.int32, (heads, span), 1) + start
        lane = lax.broadcasted_iota(jnp.int32, (heads, 128), 1)
        scores = []
        for j in range(GROUP):
            at, end = pos[base + j], length[base + j]
            s = lax.dot_general(q[j].astype(BF16), k_buf[base + j], (((1,), (1,)), ((), ())), preferred_element_type=F32)
            scores.append(jnp.where(jnp.logical_and(col < end, col != at), s * dim ** -0.5, -jnp.inf))
        probs, extra = [], []
        stats = ml[k]
        for j in range(GROUP):
            at, end = pos[base + j], length[base + j]
            owned = jnp.logical_and(jnp.logical_and(at >= start, at < start + span), at < end)
            s_new = jnp.where(owned, fresh[j], -jnp.inf)
            m = jnp.maximum(jnp.maximum(jnp.max(scores[j], axis=1, keepdims=True), s_new), NEG_FLOOR)
            p, p_new = jnp.exp(scores[j] - m), jnp.exp(s_new - m)
            spot = base + j - CHUNKS[k][0]
            stats = jnp.where(lane == spot, m, stats)
            stats = jnp.where(lane == 64 + spot, jnp.sum(p, axis=1, keepdims=True) + p_new, stats)
            probs.append(p.astype(BF16))
            extra.append(p_new)
        ml[k] = stats
        out = [jnp.dot(probs[j], v_buf[base + j], preferred_element_type=F32) + extra[j] * v_row[base + j:base + j + 1, :]
               for j in range(GROUP)]
        acc[:, here, :] = jnp.swapaxes(jnp.stack(out), 0, 1)

    def to(n, k, src, dst, peer):
        return pltpu.make_async_remote_copy(src_ref=src, dst_ref=dst, send_sem=send.at[n, k], recv_sem=recv.at[n, k],
                                            device_id={'sp': peer}, device_id_type=MESH)

    def heads_of(xx, cc):
        return 4 * xx + 2 * cc

    def col_of(v, h):
        lane = lax.broadcasted_iota(jnp.int32, v.shape, 1)
        return jnp.sum(jnp.where(lane == h, v, 0.0), axis=1, keepdims=True)

    def copy_of(n, k):
        r0, r1 = CHUNKS[k]
        rs = pl.ds(r0, r1 - r0)
        if n < 3:
            return to(n, k, ml.at[k], ml_in.at[n, k], (pair, across, far)[n])
        if n == 3:
            return to(n, k, acc.at[pl.ds(heads_of(1 - x, 1 - c), 2), rs], part1.at[0, :, rs], pair)
        if n == 4:
            return to(n, k, acc.at[pl.ds(heads_of(x, 1 - c), 2), rs], part1.at[1, :, rs], pair)
        if n == 5:
            return to(n, k, send2.at[:, rs], part2.at[:, rs], across)
        if n == 6:
            return to(n, k, half.at[0, rs], part3.at[rs], pair)
        if n == 7:
            return to(n, k, send4.at[rs], part4.at[rs], across)
        return to(n, k, done.at[rs], part5.at[rs], pair)

    def stage(n, k):
        r0, r1 = CHUNKS[k]
        size = r1 - r0
        rs = slice(r0, r1)

        def split(v):
            t = v.T
            return t[:size], t[64:64 + size]

        own_cols = pl.ds(pl.multiple_of(c * wide, wide), wide)
        other_cols = pl.ds(pl.multiple_of((1 - c) * wide, wide), wide)
        if n == 0:
            if k == 0:
                pl.semaphore_wait(barrier, 3)
            for q in range(5):
                copy_of(q, k).start()
        elif n == 1:
            copy_of(0, k).wait()
            m0, m1 = split(ml[k])[0], split(ml_in[0, k])[0]
            mp = jnp.maximum(m0, m1)
            e0, e1 = jnp.exp(m0 - mp), jnp.exp(m1 - mp)
            copy_of(3, k).wait()
            for j in range(2):
                h = heads_of(1 - x, c) + j
                send2[j, rs] = acc[h, rs] * col_of(e0, h) + part1[0, j, rs] * col_of(e1, h)
            copy_of(5, k).start()
            copy_of(4, k).wait()
            for j in range(2):
                h = heads_of(x, c) + j
                mine[j, rs] = acc[h, rs] * col_of(e0, h) + part1[1, j, rs] * col_of(e1, h)
        elif n == 2:
            copy_of(1, k).wait()
            copy_of(2, k).wait()
            m0, l0 = split(ml[k])
            m1, l1 = split(ml_in[0, k])
            m2, l2 = split(ml_in[1, k])
            m3, l3 = split(ml_in[2, k])
            mp, mq = jnp.maximum(m0, m1), jnp.maximum(m2, m3)
            mt = jnp.maximum(mp, mq)
            inv = 1.0 / (l0 * jnp.exp(m0 - mt) + l1 * jnp.exp(m1 - mt) + l2 * jnp.exp(m2 - mt) + l3 * jnp.exp(m3 - mt))
            ep, eq = jnp.exp(mp - mt) * inv, jnp.exp(mq - mt) * inv
            heads_here = [heads_of(x, c) + j for j in range(2)]
            factors = [(col_of(ep, h), col_of(eq, h)) for h in heads_here]
            if k == 0:
                last.wait()
            copy_of(5, k).wait()
            o = jnp.concatenate([(mine[j, rs] * factors[j][0] + part2[j, rs] * factors[j][1]).astype(BF16) for j in range(2)], axis=1)
            half[0, rs] = jnp.dot(o, wo[:, other_cols], preferred_element_type=F32)
            copy_of(6, k).start()
            half[1, rs] = jnp.dot(o, wo[:, own_cols], preferred_element_type=F32)
        elif n == 3:
            copy_of(6, k).wait()
            send4[rs] = half[1, rs] + part3[rs]
            copy_of(7, k).start()
        elif n == 4:
            copy_of(7, k).wait()
            done[rs] = (send4[rs] + part4[rs]).astype(BF16)
            copy_of(8, k).start()
            att[rs, own_cols] = done[rs]
        else:
            copy_of(8, k).wait()
            att[rs, other_cols] = part5[rs]

    for k in range(len(CHUNKS)):
        ml[k] = jnp.zeros(ml.shape[1:], F32)
    for g in range(groups):
        group_step(g, [k for k, (r0, r1) in enumerate(CHUNKS) if r0 <= g * GROUP < r1][0])
        for n, k in PLAN.get(g, ()):
            stage(n, k)
    for n, k in PLAN[groups]:
        stage(n, k)


def store(k_in, v_in, k_row, v_row, att, pos, k_out, v_out, att_out, k_buf, v_buf, sem_k, sem_v, sem_a):
    rows, span, dim = k_in.shape
    groups = rows // GROUP
    start = lax.axis_index('sp') * span
    tail = pltpu.make_async_copy(att, att_out, sem_a)
    tail.start()
    sub = lax.broadcasted_iota(jnp.int32, (16, dim), 0)

    def patch(g):
        for b in range(g * GROUP, (g + 1) * GROUP):
            at = pos[b] - start
            inside = jnp.logical_and(at >= 0, at < span)
            at = jnp.where(inside, at, 0)
            win = pl.ds(pl.multiple_of(at // 16 * 16, 16), 16)
            hit = jnp.logical_and(sub == at % 16, inside)
            for row, buf in ((k_row, k_buf), (v_row, v_buf)):
                buf[b, win, :] = jnp.where(hit, row[b:b + 1, :], buf[b, win, :].astype(F32)).astype(BF16)

    def put(g):
        part = pl.ds(g * GROUP, GROUP)
        return (pltpu.make_async_copy(k_buf.at[part], k_out.at[part], sem_k.at[g]),
                pltpu.make_async_copy(v_buf.at[part], v_out.at[part], sem_v.at[g]))

    patch(0)
    for g in range(groups):
        if g + 1 < groups:
            patch(g + 1)
        for copy in put(g):
            copy.start()
    for g in range(groups):
        for copy in put(g):
            copy.wait()
    tail.wait()


def solution(mesh):
    row_spec = P(('rep', 'dp'), None)
    cache_spec = P(('rep', 'dp'), 'sp', None, None)
    len_spec = P(('rep', 'dp'))

    def local_step(hidden, w_query, w_key, w_value, w_out, k_cache, v_cache, write_pos, valid_len):
        rows, span, kv_heads, dim = k_cache.shape
        model = hidden.shape[1]
        heads = w_query.shape[1] // dim
        cache = (rows, span, dim)
        wide = w_out.shape[1] // 2
        pair = (2, rows, dim)
        chunks = len(CHUNKS)
        dma = pltpu.SemaphoreType.DMA
        hbm = lambda a: pltpu.with_memory_space_constraint(a, pltpu.HBM)
        vm = lambda a: pltpu.with_memory_space_constraint(a, pltpu.VMEM)
        att, k_mid, v_mid, k_row, v_row = pl.pallas_call(
            attend,
            out_shape=[pltpu.VMEM((rows, w_out.shape[1]), BF16), pltpu.VMEM(cache, BF16), pltpu.VMEM(cache, BF16),
                       pltpu.VMEM((rows, dim), F32), pltpu.VMEM((rows, dim), F32)],
            in_specs=[ANY] * 9,
            out_specs=[VMEM] * 5,
            scratch_shapes=[pltpu.VMEM((rows, model), BF16), pltpu.VMEM(w_query.shape, BF16),
                            pltpu.VMEM(w_key.shape, BF16), pltpu.VMEM(w_value.shape, BF16), pltpu.VMEM(w_out.shape, BF16),
                            pltpu.VMEM((heads, rows, dim), F32),
                            pltpu.SMEM((rows,), jnp.int32), pltpu.SMEM((rows,), jnp.int32),
                            pltpu.VMEM((heads, rows, dim), F32), pltpu.VMEM((chunks, heads, 128), F32), pltpu.VMEM((3, chunks, heads, 128), F32),
                            pltpu.VMEM((2,) + pair, F32), pltpu.VMEM(pair, F32), pltpu.VMEM(pair, F32), pltpu.VMEM(pair, F32),
                            pltpu.VMEM((2, rows, wide), F32), pltpu.VMEM((rows, wide), F32), pltpu.VMEM((rows, wide), F32),
                            pltpu.VMEM((rows, wide), F32), pltpu.VMEM((rows, wide), BF16), pltpu.VMEM((rows, wide), BF16),
                            dma((4 + heads,)), dma((2,)), dma((rows // GROUP,)), dma((rows // GROUP,)), dma((9, chunks)), dma((9, chunks))],
            compiler_params=pltpu.CompilerParams(collective_id=0, has_side_effects=True, vmem_limit_bytes=24 * 2 ** 20),
            cost_estimate=pl.CostEstimate(flops=10 ** 9, bytes_accessed=46 * 10 ** 6, transcendentals=0),
            name='attend',
        )(*map(hbm, (hidden, w_query, w_key, w_value, w_out, k_cache.reshape(cache), v_cache.reshape(cache), write_pos, valid_len)))
        k_new, v_new, attn_out, _, _ = pl.pallas_call(
            store,
            out_shape=[pltpu.HBM(cache, BF16), pltpu.HBM(cache, BF16), pltpu.HBM(att.shape, BF16), pltpu.VMEM(cache, BF16), pltpu.VMEM(cache, BF16)],
            in_specs=[VMEM] * 5 + [SMEM],
            out_specs=[ANY, ANY, ANY, VMEM, VMEM],
            input_output_aliases={0: 3, 1: 4},
            scratch_shapes=[dma((rows // GROUP,)), dma((rows // GROUP,)), dma],
            compiler_params=pltpu.CompilerParams(vmem_limit_bytes=24 * 2 ** 20),
            cost_estimate=pl.CostEstimate(flops=10 ** 6, bytes_accessed=34 * 10 ** 6, transcendentals=0),
            name='store',
        )(vm(k_mid), vm(v_mid), vm(k_row), vm(v_row), vm(att), write_pos)
        return attn_out, k_new.reshape(k_cache.shape), v_new.reshape(v_cache.shape)

    return jax.shard_map(local_step, mesh=mesh, in_specs=(row_spec, P(), P(), P(), P('sp', None), cache_spec, cache_spec, len_spec, len_spec), out_specs=(row_spec, cache_spec, cache_spec), check_vma=False)
```

```python
import functools

import jax
import jax.numpy as jnp
from jax import lax
from jax.experimental import pallas as pl
from jax.experimental.pallas import tpu as pltpu
from jax.sharding import PartitionSpec as P


F32, BF16 = jnp.float32, jnp.bfloat16
NEG_FLOOR = -1e30
GROUP = 8
FEED = (1, 1, 2, 2, 2, 2, 2)
LATE = 4
CHUNKS = ((0, 48), (48, 64))
TAIL = ((2, 0), (3, 0), (2, 1), (3, 1))
SPLIT = 16
EARLY = 2
ANY = pl.BlockSpec(memory_space=pl.ANY)
VMEM = pl.BlockSpec(memory_space=pltpu.VMEM)
SMEM = pl.BlockSpec(memory_space=pltpu.SMEM)
MESH = pl.DeviceIdType.MESH


def attend(hid_hbm, wq_hbm, wk_hbm, wv_hbm, wo_hbm, k_hbm, v_hbm, pos_hbm, len_hbm,
           total, k_buf, v_buf, kv_row,
           hid, wq, wkv, wo, q_all, pos, length, acc, ml, ml_in, parts, half, part3,
           sem_w, sem_s, sem_k, sem_v, send_q, recv_q, send_a, recv_a, send, recv):
    rows, span, dim = k_buf.shape
    heads = q_all.shape[0]
    groups = rows // GROUP
    wide = half.shape[2]
    mine = heads // 2
    i = lax.axis_index('sp')
    x, c = i // 2, i % 2
    peers = pair, across, far = 2 * x + 1 - c, 2 * (1 - x) + c, 2 * (1 - x) + 1 - c
    start = i * span
    barrier = pltpu.get_barrier_semaphore()
    for peer in peers:
        pl.semaphore_signal(barrier, inc=1, device_id={'sp': peer}, device_id_type=MESH)

    def fetch(kind, g):
        part = pl.ds(g * GROUP, GROUP)
        if kind == 'o':
            return pltpu.make_async_copy(wo_hbm, wo, sem_w.at[2])
        if kind == 'k':
            return pltpu.make_async_copy(k_hbm.at[part], k_buf.at[part], sem_k.at[g])
        return pltpu.make_async_copy(v_hbm.at[part], v_buf.at[part], sem_v.at[g])

    def q_part(h):
        cols = pl.ds(pl.multiple_of((c * mine + h) * dim, dim), dim)
        return pltpu.make_async_copy(wq_hbm.at[:, cols], wq.at[h], sem_w.at[3 + h])

    def kv_part(hbm):
        return pltpu.make_async_copy(hbm, wkv, sem_w.at[1])

    def to(src, dst, sems, at, peer):
        return pltpu.make_async_remote_copy(src_ref=src, dst_ref=dst, send_sem=sems[0].at[at], recv_sem=sems[1].at[at],
                                            device_id={'sp': peer}, device_id_type=MESH)

    def heads_of(peer):
        return 2 * peer

    scal = [pltpu.make_async_copy(pos_hbm, pos, sem_s.at[0]), pltpu.make_async_copy(len_hbm, length, sem_s.at[1])]
    hidden = pltpu.make_async_copy(hid_hbm, hid, sem_w.at[0])
    hidden.start()

    @pl.when(c == 0)
    def _():
        kv_part(wk_hbm).start()

    @pl.when(c == 1)
    def _():
        kv_part(wv_hbm).start()

    for h in range(mine):
        q_part(h).start()
    for copy in scal:
        copy.start()
    order = [('k', 0)]
    for g in range(1, groups):
        order += [('k', g), ('v', g - 1)]
    order.append(('v', groups - 1))
    order.insert(2 * LATE, ('o', 0))
    started = []

    def begin(count):
        for item in order[len(started):len(started) + count]:
            started.append(item)
            fetch(*item).start()

    begin(FEED[0])
    for copy in scal:
        copy.wait()
    hidden.wait()
    kv_part(wk_hbm).wait()
    begin(FEED[1])
    kv_row[c] = jnp.dot(hid[...], wkv[...], preferred_element_type=F32).astype(BF16).astype(F32)
    for h in range(mine):
        q_part(h).wait()
        begin(FEED[2 + h])
        q_all[c * mine + h] = jnp.dot(hid[...], wq[h], preferred_element_type=F32).astype(BF16).astype(F32)
    for k in range(len(CHUNKS)):
        ml[k] = jnp.zeros(ml.shape[1:], F32)
    pl.semaphore_wait(barrier, 3)
    q_half = q_all.at[pl.ds(c * mine, mine)]
    swaps = [to(kv_row.at[c], kv_row.at[c], (send_q, recv_q), 0, pair), to(q_half, q_half, (send_q, recv_q), 1, pair)]
    for copy in swaps:
        copy.start()
    for copy in swaps:
        copy.wait()

    def score(g):
        base = g * GROUP
        here = slice(base, base + GROUP)
        k = [n for n, (r0, r1) in enumerate(CHUNKS) if r0 <= base < r1][0]
        q = jnp.swapaxes(q_all[:, here, :], 0, 1)
        fresh = jnp.sum(q * kv_row[0, here, :][:, None, :], axis=2, keepdims=True) * dim ** -0.5
        col = lax.broadcasted_iota(jnp.int32, (heads, span), 1) + start
        lane = lax.broadcasted_iota(jnp.int32, (heads, 128), 1)
        scores = []
        for j in range(GROUP):
            at, end = pos[base + j], length[base + j]
            s = lax.dot_general(q[j].astype(BF16), k_buf[base + j], (((1,), (1,)), ((), ())), preferred_element_type=F32)
            scores.append(jnp.where(jnp.logical_and(col < end, col != at), s * dim ** -0.5, -jnp.inf))
        probs, extra = [], []
        stats = ml[k]
        for j in range(GROUP):
            at, end = pos[base + j], length[base + j]
            owned = jnp.logical_and(jnp.logical_and(at >= start, at < start + span), at < end)
            s_new = jnp.where(owned, fresh[j], -jnp.inf)
            m = jnp.maximum(jnp.maximum(jnp.max(scores[j], axis=1, keepdims=True), s_new), NEG_FLOOR)
            p, p_new = jnp.exp(scores[j] - m), jnp.exp(s_new - m)
            spot = base + j - CHUNKS[k][0]
            stats = jnp.where(lane == spot, m, stats)
            stats = jnp.where(lane == 64 + spot, jnp.sum(p, axis=1, keepdims=True) + p_new, stats)
            probs.append(p.astype(BF16))
            extra.append(p_new)
        ml[k] = stats
        return probs, extra

    def blend(g, probs, extra):
        base = g * GROUP
        out = [jnp.dot(probs[j], v_buf[base + j], preferred_element_type=F32) + extra[j] * kv_row[1, base + j:base + j + 1, :]
               for j in range(GROUP)]
        acc[:, base:base + GROUP, :] = jnp.swapaxes(jnp.stack(out), 0, 1)

    def give_acc(g, n):
        rs = pl.ds(g * GROUP, GROUP)
        return to(acc.at[pl.ds(heads_of(peers[n]), 2), rs], parts.at[n, :, rs], (send_a, recv_a), (n, g), peers[n])

    def give(n, k):
        r0, r1 = CHUNKS[k]
        rs = pl.ds(r0, r1 - r0)
        sems = send, recv
        if n < 3:
            return to(ml.at[k], ml_in.at[n, k], sems, (n, k), peers[n])
        return to(half.at[0, rs], part3.at[rs], sems, (n, k), pair)

    own_cols = pl.ds(pl.multiple_of(c * wide, wide), wide)
    other_cols = pl.ds(pl.multiple_of((1 - c) * wide, wide), wide)

    def col_of(v, h):
        lane = lax.broadcasted_iota(jnp.int32, v.shape, 1)
        return jnp.sum(jnp.where(lane == h, v, 0.0), axis=1, keepdims=True)

    def stage(n, k):
        r0, r1 = CHUNKS[k]
        size = r1 - r0
        rs = slice(r0, r1)
        if n == 2:
            for q in range(3):
                give(q, k).wait()
            stats = []
            for v in (ml[k], ml_in[0, k], ml_in[1, k], ml_in[2, k]):
                t = v.T
                stats.append((t[:size], t[64:64 + size]))
            top = functools.reduce(jnp.maximum, [m for m, _ in stats])
            scale = [jnp.exp(m - top) for m, _ in stats]
            inv = 1.0 / functools.reduce(jnp.add, [l * e for (_, l), e in zip(stats, scale)])
            scale = [e * inv for e in scale]
            cols = [[col_of(e, heads_of(i) + j) for e in scale] for j in range(2)]
            if k == 0:
                fetch('o', 0).wait()
            for q in range(3):
                for g in range(r0 // GROUP, r1 // GROUP):
                    give_acc(g, q).wait()
            o = []
            for j in range(2):
                part = acc[heads_of(i) + j, rs] * cols[j][0]
                for q in range(3):
                    part += parts[q, j, rs] * cols[j][q + 1]
                o.append(part.astype(BF16))
            o = jnp.concatenate(o, axis=1)
            half[0, rs] = jnp.dot(o, wo[:, other_cols], preferred_element_type=F32)
            give(3, k).start()
            half[1, rs] = jnp.dot(o, wo[:, own_cols], preferred_element_type=F32)
        else:
            give(3, k).wait()
            total[rs] = half[1, rs] + part3[rs]

    fetch('k', 0).wait()
    held = score(0)
    for g in range(groups):
        if g + 1 < groups:
            fetch('k', g + 1).wait()
        fetch('v', g).wait()
        begin(FEED[-1])
        following = score(g + 1) if g + 1 < groups else None
        blend(g, *held)
        held = following
        for n in range(3):
            give_acc(g, n).start()
        for k, (r0, r1) in enumerate(CHUNKS):
            if r1 == (g + 1) * GROUP:
                for n in range(3):
                    give(n, k).start()
    for n, k in TAIL:
        stage(n, k)


def store(jobs, kv_row, pos_hbm, bufs, outs, pos, sem_p, sem_g, sem_w):
    span, dim = bufs[0].shape[1:]
    start = lax.axis_index('sp') * span
    sub = lax.broadcasted_iota(jnp.int32, (16, dim), 0)
    cuts = [(n, r) for n, r0, r1 in jobs for r in range(r0, r1, GROUP)]

    def place(b):
        at = pos[b] - start
        inside = jnp.logical_and(at >= 0, at < span)
        at = jnp.where(inside, at, 0)
        return at, inside, pl.ds(pl.multiple_of(at // 16 * 16, 16), 16)

    def patch(n, r):
        for b in range(r, r + GROUP):
            at, inside, win = place(b)
            hit = jnp.logical_and(sub == at % 16, inside)
            bufs[n][b, win, :] = jnp.where(hit, kv_row[n, b:b + 1, :], bufs[n][b, win, :].astype(F32)).astype(BF16)

    def put(n, r):
        part = pl.ds(r, GROUP)
        return pltpu.make_async_copy(bufs[n].at[part], outs[n].at[part], sem_g.at[n, r // GROUP])

    def windows(n, r, act):
        for b in range(r, r + GROUP):
            _, inside, win = place(b)

            @pl.when(inside)
            def _():
                act(pltpu.make_async_copy(bufs[n].at[b, win], outs[n].at[b, win], sem_w.at[b - cuts[0][1]]))

    ask = pltpu.make_async_copy(pos_hbm, pos, sem_p)
    ask.start()
    early, later = cuts[:EARLY], cuts[EARLY:]
    for cut in early:
        put(*cut).start()
    ask.wait()
    for cut in later:
        patch(*cut)
        put(*cut).start()
    for cut in early:
        put(*cut).wait()
        patch(*cut)
        windows(*cut, lambda copy: copy.start())
    for cut in later:
        put(*cut).wait()
    for cut in early:
        windows(*cut, lambda copy: copy.wait())


def store_first(k_in, v_in, kv_row, pos_hbm, k_out, v_out, k_buf, v_buf, *rest, jobs):
    store(jobs, kv_row, pos_hbm, (k_buf, v_buf), (k_out, v_out), *rest)


def store_second(v_in, kv_row, pos_hbm, v_old, v_out, v_buf, *rest, jobs):
    store(jobs, kv_row, pos_hbm, (v_buf, v_buf), (v_out, v_out), *rest)


def final(own, other, pair_own, pair_other, out):
    wide = own.shape[1]
    c = lax.axis_index('sp') % 2
    out[:, pl.ds(pl.multiple_of(c * wide, wide), wide)] = (own[...] + other[...]).astype(BF16)
    out[:, pl.ds(pl.multiple_of((1 - c) * wide, wide), wide)] = (pair_own[...] + pair_other[...]).astype(BF16)


def solution(mesh):
    row_spec = P(('rep', 'dp'), None)
    cache_spec = P(('rep', 'dp'), 'sp', None, None)
    len_spec = P(('rep', 'dp'))

    def one_step(hidden, w_query, w_key, w_value, w_out, k_cache, v_cache, write_pos, valid_len):
        rows, span, _, dim = k_cache.shape
        model = hidden.shape[1]
        heads = w_query.shape[1] // dim
        cache = (rows, span, dim)
        wide = w_out.shape[1] // 2
        pair = (2, rows, dim)
        chunks = len(CHUNKS)
        dma = pltpu.SemaphoreType.DMA
        hbm = lambda a: pltpu.with_memory_space_constraint(a, pltpu.HBM)
        vm = lambda a: pltpu.with_memory_space_constraint(a, pltpu.VMEM)
        total, k_mid, v_mid, kv_row = pl.pallas_call(
            attend,
            out_shape=[pltpu.VMEM((rows, wide), F32), pltpu.VMEM(cache, BF16), pltpu.VMEM(cache, BF16),
                       pltpu.VMEM((2, rows, dim), F32)],
            in_specs=[ANY] * 9,
            out_specs=[VMEM] * 4,
            scratch_shapes=[pltpu.VMEM((rows, model), BF16), pltpu.VMEM((heads // 2, model, dim), BF16),
                            pltpu.VMEM(w_key.shape, BF16), pltpu.VMEM(w_out.shape, BF16),
                            pltpu.VMEM((heads, rows, dim), F32),
                            pltpu.SMEM((rows,), jnp.int32), pltpu.SMEM((rows,), jnp.int32),
                            pltpu.VMEM((heads, rows, dim), F32), pltpu.VMEM((chunks, heads, 128), F32), pltpu.VMEM((3, chunks, heads, 128), F32),
                            pltpu.VMEM((3,) + pair, F32),
                            pltpu.VMEM((2, rows, wide), F32), pltpu.VMEM((rows, wide), F32),
                            dma((3 + heads // 2,)), dma((2,)), dma((rows // GROUP,)), dma((rows // GROUP,)), dma((2,)), dma((2,)),
                            dma((3, rows // GROUP)), dma((3, rows // GROUP)), dma((4, chunks)), dma((4, chunks))],
            compiler_params=pltpu.CompilerParams(collective_id=0, has_side_effects=True, vmem_limit_bytes=12 * 2 ** 20),
            cost_estimate=pl.CostEstimate(flops=10 ** 9, bytes_accessed=46 * 10 ** 6, transcendentals=0),
            name='attend',
        )(*map(hbm, (hidden, w_query, w_key, w_value, w_out, k_cache.reshape(cache), v_cache.reshape(cache), write_pos, valid_len)))
        across = [(d, (d + 2) % 4) for d in range(4)]
        pairs = [(d, d ^ 1) for d in range(4)]
        other = lax.ppermute(total, 'sp', across)
        pair_own = lax.ppermute(total, 'sp', pairs)
        pair_other = lax.ppermute(other, 'sp', pairs)
        common = dict(
            scratch_shapes=[pltpu.SMEM((rows,), jnp.int32), dma, dma((2, rows // GROUP)), dma((EARLY * GROUP,))],
            compiler_params=pltpu.CompilerParams(vmem_limit_bytes=12 * 2 ** 20))
        full, held = pltpu.HBM(cache, BF16), pltpu.VMEM(cache, BF16)
        k_new, v_part, _, v_mid = pl.pallas_call(
            functools.partial(store_first, jobs=((0, 0, rows), (1, 0, SPLIT))),
            out_shape=[full, full, held, held], in_specs=[VMEM] * 3 + [ANY], out_specs=[ANY, ANY, VMEM, VMEM],
            input_output_aliases={0: 2, 1: 3}, name='store_first',
            cost_estimate=pl.CostEstimate(flops=10 ** 9, bytes_accessed=21 * 10 ** 6, transcendentals=0), **common,
        )(vm(k_mid), vm(v_mid), vm(kv_row), hbm(write_pos))
        v_new, _ = pl.pallas_call(
            functools.partial(store_second, jobs=((1, SPLIT, rows),)),
            out_shape=[full, held], in_specs=[VMEM, VMEM, ANY, ANY], out_specs=[ANY, VMEM],
            input_output_aliases={0: 1, 3: 0}, name='store_second',
            cost_estimate=pl.CostEstimate(flops=6 * 10 ** 8, bytes_accessed=13 * 10 ** 6, transcendentals=0), **common,
        )(vm(v_mid), vm(kv_row), hbm(write_pos), v_part)
        attn_out = pl.pallas_call(
            final,
            out_shape=jax.ShapeDtypeStruct((rows, w_out.shape[1]), BF16),
            in_specs=[VMEM] * 4,
            out_specs=VMEM,
            compiler_params=pltpu.CompilerParams(vmem_limit_bytes=4 * 2 ** 20),
            cost_estimate=pl.CostEstimate(flops=10 ** 6, bytes_accessed=2 ** 20, transcendentals=0),
            name='final',
        )(total, other, pair_own, pair_other)
        return attn_out, k_new.reshape(k_cache.shape), v_new.reshape(v_cache.shape)

    return jax.shard_map(one_step, mesh=mesh, in_specs=(row_spec, P(), P(), P(), P('sp', None), cache_spec, cache_spec, len_spec, len_spec), out_specs=(row_spec, cache_spec, cache_spec), check_vma=False)
```

```python
import functools

import jax
import jax.numpy as jnp
from jax import lax
from jax.experimental import pallas as pl
from jax.experimental.pallas import tpu as pltpu
from jax.sharding import PartitionSpec as P


F32, BF16 = jnp.float32, jnp.bfloat16
NEG_FLOOR = -1e30
GROUP = 8
FEED = (1, 1, 2, 2, 2, 2, 2)
LATE = 6
CHUNKS = ((0, 48), (48, 64))
SPLIT = 48
EARLY = 1
ANY = pl.BlockSpec(memory_space=pl.ANY)
VMEM = pl.BlockSpec(memory_space=pltpu.VMEM)
SMEM = pl.BlockSpec(memory_space=pltpu.SMEM)
MESH = pl.DeviceIdType.MESH


def attend(hid_hbm, wq_hbm, wk_hbm, wv_hbm, wo_hbm, k_hbm, v_hbm, pos_hbm, len_hbm,
           total, k_buf, v_buf, kv_row,
           hid, wq, wkv, wo, q_all, pos, length, acc, ml, ml_in, parts, half, part3,
           sem_w, sem_s, sem_k, sem_v, send_q, recv_q, send_a, recv_a, send, recv):
    rows, span, dim = k_buf.shape
    heads = q_all.shape[0]
    groups = rows // GROUP
    wide = half.shape[1]
    mine = heads // 2
    i = lax.axis_index('sp')
    x, c = i // 2, i % 2
    peers = pair, across, far = 2 * x + 1 - c, 2 * (1 - x) + c, 2 * (1 - x) + 1 - c
    start = i * span
    barrier = pltpu.get_barrier_semaphore()
    for peer in peers:
        pl.semaphore_signal(barrier, inc=1, device_id={'sp': peer}, device_id_type=MESH)

    def fetch(kind, g):
        part = pl.ds(g * GROUP, GROUP)
        if kind == 'o':
            return pltpu.make_async_copy(wo_hbm, wo, sem_w.at[2])
        if kind == 'k':
            return pltpu.make_async_copy(k_hbm.at[part], k_buf.at[part], sem_k.at[g])
        if g == groups - 1:
            part = pl.ds(g * GROUP + (kind == 'w') * GROUP // 2, GROUP // 2)
        return pltpu.make_async_copy(v_hbm.at[part], v_buf.at[part], sem_v.at[g + (kind == 'w')])

    def q_part(h):
        cols = pl.ds(pl.multiple_of((c * mine + h) * dim, dim), dim)
        return pltpu.make_async_copy(wq_hbm.at[:, cols], wq.at[h], sem_w.at[3 + h])

    def kv_part(hbm):
        return pltpu.make_async_copy(hbm, wkv, sem_w.at[1])

    def to(src, dst, sems, at, peer):
        return pltpu.make_async_remote_copy(src_ref=src, dst_ref=dst, send_sem=sems[0].at[at], recv_sem=sems[1].at[at],
                                            device_id={'sp': peer}, device_id_type=MESH)

    def heads_of(peer):
        return 2 * peer

    scal = [pltpu.make_async_copy(pos_hbm, pos, sem_s.at[0]), pltpu.make_async_copy(len_hbm, length, sem_s.at[1])]
    hidden = pltpu.make_async_copy(hid_hbm, hid, sem_w.at[0])
    hidden.start()

    @pl.when(c == 0)
    def _():
        kv_part(wk_hbm).start()

    @pl.when(c == 1)
    def _():
        kv_part(wv_hbm).start()

    for h in range(mine):
        q_part(h).start()
    for copy in scal:
        copy.start()
    order = [('k', 0)]
    for g in range(1, groups):
        order += [('k', g), ('v', g - 1)]
    order += [('v', groups - 1), ('w', groups - 1)]
    order.insert(2 * LATE, ('o', 0))
    started = []

    def begin(count):
        for item in order[len(started):len(started) + count]:
            started.append(item)
            fetch(*item).start()

    begin(FEED[0])
    for copy in scal:
        copy.wait()
    hidden.wait()
    kv_part(wk_hbm).wait()
    begin(FEED[1])
    kv_row[c] = jnp.dot(hid[...], wkv[...], preferred_element_type=F32).astype(BF16).astype(F32)
    for h in range(mine):
        q_part(h).wait()
        begin(FEED[2 + h])
        q_all[c * mine + h] = jnp.dot(hid[...], wq[h], preferred_element_type=F32).astype(BF16).astype(F32)
    for k in range(len(CHUNKS)):
        ml[k] = jnp.zeros(ml.shape[1:], F32)
    pl.semaphore_wait(barrier, 3)
    q_half = q_all.at[pl.ds(c * mine, mine)]
    swaps = [to(kv_row.at[c], kv_row.at[c], (send_q, recv_q), 0, pair), to(q_half, q_half, (send_q, recv_q), 1, pair)]
    for copy in swaps:
        copy.start()
    for copy in swaps:
        copy.wait()

    def score(g):
        base = g * GROUP
        here = slice(base, base + GROUP)
        k = [n for n, (r0, r1) in enumerate(CHUNKS) if r0 <= base < r1][0]
        q = jnp.swapaxes(q_all[:, here, :], 0, 1)
        fresh = jnp.sum(q * kv_row[0, here, :][:, None, :], axis=2, keepdims=True) * dim ** -0.5
        col = lax.broadcasted_iota(jnp.int32, (heads, span), 1) + start
        lane = lax.broadcasted_iota(jnp.int32, (heads, 128), 1)
        scores = []
        for j in range(GROUP):
            at, end = pos[base + j], length[base + j]
            s = lax.dot_general(q[j].astype(BF16), k_buf[base + j], (((1,), (1,)), ((), ())), preferred_element_type=F32)
            scores.append(jnp.where(jnp.logical_and(col < end, col != at), s * dim ** -0.5, -jnp.inf))
        probs, extra = [], []
        stats = ml[k]
        for j in range(GROUP):
            at, end = pos[base + j], length[base + j]
            owned = jnp.logical_and(jnp.logical_and(at >= start, at < start + span), at < end)
            s_new = jnp.where(owned, fresh[j], -jnp.inf)
            m = jnp.maximum(jnp.maximum(jnp.max(scores[j], axis=1, keepdims=True), s_new), NEG_FLOOR)
            p, p_new = jnp.exp(scores[j] - m), jnp.exp(s_new - m)
            spot = base + j - CHUNKS[k][0]
            stats = jnp.where(lane == spot, m, stats)
            stats = jnp.where(lane == 64 + spot, jnp.sum(p, axis=1, keepdims=True) + p_new, stats)
            probs.append(p.astype(BF16))
            extra.append(p_new)
        ml[k] = stats
        return probs, extra

    def blend(g, probs, extra):
        base = g * GROUP
        out = []
        for j in range(GROUP):
            if g == groups - 1 and j == GROUP // 2:
                fetch('w', g).wait()
            out.append(jnp.dot(probs[j], v_buf[base + j], preferred_element_type=F32) + extra[j] * kv_row[1, base + j:base + j + 1, :])
        acc[:, base:base + GROUP, :] = jnp.swapaxes(jnp.stack(out), 0, 1)

    def give_acc(g, n):
        rs = pl.ds(g * GROUP, GROUP)
        return to(acc.at[pl.ds(heads_of(peers[n]), 2), rs], parts.at[n, :, rs], (send_a, recv_a), (n, g), peers[n])

    def give(n, k):
        r0, r1 = CHUNKS[k]
        rs = pl.ds(r0, r1 - r0)
        sems = send, recv
        if n < 3:
            return to(ml.at[k], ml_in.at[n, k], sems, (n, k), peers[n])
        return to(half, part3, sems, (n, k), pair)

    own_cols = pl.ds(pl.multiple_of(c * wide, wide), wide)
    other_cols = pl.ds(pl.multiple_of((1 - c) * wide, wide), wide)

    def col_of(v, h):
        lane = lax.broadcasted_iota(jnp.int32, v.shape, 1)
        return jnp.sum(jnp.where(lane == h, v, 0.0), axis=1, keepdims=True)

    def combine(k):
        r0, r1 = CHUNKS[k]
        size = r1 - r0
        rs = slice(r0, r1)
        for q in range(3):
            give(q, k).wait()
        stats = []
        for v in (ml[k], ml_in[0, k], ml_in[1, k], ml_in[2, k]):
            t = v.T
            stats.append((t[:size], t[64:64 + size]))
        top = functools.reduce(jnp.maximum, [m for m, _ in stats])
        scale = [jnp.exp(m - top) for m, _ in stats]
        inv = 1.0 / functools.reduce(jnp.add, [l * e for (_, l), e in zip(stats, scale)])
        scale = [e * inv for e in scale]
        cols = [[col_of(e, heads_of(i) + j) for e in scale] for j in range(2)]
        if k == 0:
            fetch('o', 0).wait()
        for q in range(3):
            for g in range(r0 // GROUP, r1 // GROUP):
                give_acc(g, q).wait()
        o = []
        for j in range(2):
            part = acc[heads_of(i) + j, rs] * cols[j][0]
            for q in range(3):
                part += parts[q, j, rs] * cols[j][q + 1]
            o.append(part.astype(BF16))
        o = jnp.concatenate(o, axis=1)
        return o

    fetch('k', 0).wait()
    held = score(0)
    for g in range(groups):
        if g + 1 < groups:
            fetch('k', g + 1).wait()
        fetch('v', g).wait()
        begin(FEED[-1])
        following = score(g + 1) if g + 1 < groups else None
        blend(g, *held)
        held = following
        for k, (r0, r1) in enumerate(CHUNKS):
            if r1 == (g + 1) * GROUP:
                for n in (1, 2, 0):
                    give(n, k).start()
        for n in (1, 2, 0):
            give_acc(g, n).start()
    o = combine(0)
    early = CHUNKS[0][1]
    half[...] = jnp.dot(o, wo[:, other_cols], preferred_element_type=F32)
    give(3, 0).start()
    total[:early] = jnp.dot(o, wo[:, own_cols], preferred_element_type=F32)
    give(3, 0).wait()
    total[:early] += part3[...]
    o = combine(1)
    total[early:rows] = jnp.dot(o, wo[:, own_cols], preferred_element_type=F32)
    total[rows:] = jnp.dot(o, wo[:, other_cols], preferred_element_type=F32)


def store(jobs, kv_row, pos_hbm, bufs, outs, pos, sem_p, sem_g, sem_w):
    span, dim = bufs[0].shape[1:]
    start = lax.axis_index('sp') * span
    sub = lax.broadcasted_iota(jnp.int32, (16, dim), 0)
    cuts = [(n, r) for n, r0, r1 in jobs for r in range(r0, r1, GROUP)]

    def place(b):
        at = pos[b] - start
        inside = jnp.logical_and(at >= 0, at < span)
        at = jnp.where(inside, at, 0)
        return at, inside, pl.ds(pl.multiple_of(at // 16 * 16, 16), 16)

    def patch(n, r):
        for b in range(r, r + GROUP):
            at, inside, win = place(b)
            hit = jnp.logical_and(sub == at % 16, inside)
            bufs[n][b, win, :] = jnp.where(hit, kv_row[n, b:b + 1, :], bufs[n][b, win, :].astype(F32)).astype(BF16)

    def put(n, r):
        part = pl.ds(r, GROUP)
        return pltpu.make_async_copy(bufs[n].at[part], outs[n].at[part], sem_g.at[n, r // GROUP])

    def windows(n, r, act):
        for b in range(r, r + GROUP):
            _, inside, win = place(b)

            @pl.when(inside)
            def _():
                act(pltpu.make_async_copy(bufs[n].at[b, win], outs[n].at[b, win], sem_w.at[b - cuts[0][1]]))

    ask = pltpu.make_async_copy(pos_hbm, pos, sem_p)
    ask.start()
    early, later = cuts[:EARLY], cuts[EARLY:]
    for cut in early:
        put(*cut).start()
    ask.wait()
    for cut in later:
        patch(*cut)
        put(*cut).start()
    for cut in early:
        put(*cut).wait()
        patch(*cut)
        windows(*cut, lambda copy: copy.start())
    for cut in later:
        put(*cut).wait()
    for cut in early:
        windows(*cut, lambda copy: copy.wait())


def store_first(k_in, v_in, kv_row, pos_hbm, k_out, v_out, k_buf, v_buf, *rest, jobs):
    store(jobs, kv_row, pos_hbm, (k_buf, v_buf), (k_out, v_out), *rest)


def store_second(v_in, kv_row, pos_hbm, v_old, v_out, v_buf, *rest, jobs):
    store(jobs, kv_row, pos_hbm, (v_buf, v_buf), (v_out, v_out), *rest)


def final(own, other, pair_own, pair_other, out):
    rows, wide = out.shape[0], own.shape[1]
    early = CHUNKS[0][1]
    c = lax.axis_index('sp') % 2
    own_cols = pl.ds(pl.multiple_of(c * wide, wide), wide)
    other_cols = pl.ds(pl.multiple_of((1 - c) * wide, wide), wide)
    a, b = slice(early, rows), slice(rows, 2 * rows - early)
    out[:early, own_cols] = (own[:early] + other[:early]).astype(BF16)
    out[:early, other_cols] = (pair_own[:early] + pair_other[:early]).astype(BF16)
    out[early:, own_cols] = ((own[a] + pair_own[b]) + (other[a] + pair_other[b])).astype(BF16)
    out[early:, other_cols] = ((own[b] + pair_own[a]) + (other[b] + pair_other[a])).astype(BF16)


def solution(mesh):
    row_spec = P(('rep', 'dp'), None)
    cache_spec = P(('rep', 'dp'), 'sp', None, None)
    len_spec = P(('rep', 'dp'))

    def one_step(hidden, w_query, w_key, w_value, w_out, k_cache, v_cache, write_pos, valid_len):
        rows, span, _, dim = k_cache.shape
        model = hidden.shape[1]
        heads = w_query.shape[1] // dim
        cache = (rows, span, dim)
        wide = w_out.shape[1] // 2
        pair = (2, rows, dim)
        chunks = len(CHUNKS)
        dma = pltpu.SemaphoreType.DMA
        hbm = lambda a: pltpu.with_memory_space_constraint(a, pltpu.HBM)
        vm = lambda a: pltpu.with_memory_space_constraint(a, pltpu.VMEM)
        total, k_mid, v_mid, kv_row = pl.pallas_call(
            attend,
            out_shape=[pltpu.VMEM((2 * rows - CHUNKS[0][1], wide), F32), pltpu.VMEM(cache, BF16), pltpu.VMEM(cache, BF16),
                       pltpu.VMEM((2, rows, dim), F32)],
            in_specs=[ANY] * 9,
            out_specs=[VMEM] * 4,
            scratch_shapes=[pltpu.VMEM((rows, model), BF16), pltpu.VMEM((heads // 2, model, dim), BF16),
                            pltpu.VMEM(w_key.shape, BF16), pltpu.VMEM(w_out.shape, BF16),
                            pltpu.VMEM((heads, rows, dim), F32),
                            pltpu.SMEM((rows,), jnp.int32), pltpu.SMEM((rows,), jnp.int32),
                            pltpu.VMEM((heads, rows, dim), F32), pltpu.VMEM((chunks, heads, 128), F32), pltpu.VMEM((3, chunks, heads, 128), F32),
                            pltpu.VMEM((3,) + pair, F32),
                            pltpu.VMEM((CHUNKS[0][1], wide), F32), pltpu.VMEM((CHUNKS[0][1], wide), F32),
                            dma((3 + heads // 2,)), dma((2,)), dma((rows // GROUP,)), dma((rows // GROUP + 1,)), dma((2,)), dma((2,)),
                            dma((3, rows // GROUP)), dma((3, rows // GROUP)), dma((4, chunks)), dma((4, chunks))],
            compiler_params=pltpu.CompilerParams(collective_id=0, has_side_effects=True, vmem_limit_bytes=12 * 2 ** 20),
            cost_estimate=pl.CostEstimate(flops=10 ** 9, bytes_accessed=46 * 10 ** 6, transcendentals=0),
            name='attend',
        )(*map(hbm, (hidden, w_query, w_key, w_value, w_out, k_cache.reshape(cache), v_cache.reshape(cache), write_pos, valid_len)))
        across = [(d, (d + 2) % 4) for d in range(4)]
        pairs = [(d, d ^ 1) for d in range(4)]
        other = lax.ppermute(total, 'sp', across)
        pair_own = lax.ppermute(total, 'sp', pairs)
        pair_other = lax.ppermute(other, 'sp', pairs)
        common = dict(
            scratch_shapes=[pltpu.SMEM((rows,), jnp.int32), dma, dma((2, rows // GROUP)), dma((EARLY * GROUP,))],
            compiler_params=pltpu.CompilerParams(vmem_limit_bytes=12 * 2 ** 20))
        full, held = pltpu.HBM(cache, BF16), pltpu.VMEM(cache, BF16)
        k_new, v_part, _, v_mid = pl.pallas_call(
            functools.partial(store_first, jobs=((0, 0, rows), (1, 0, SPLIT))),
            out_shape=[full, full, held, held], in_specs=[VMEM] * 3 + [ANY], out_specs=[ANY, ANY, VMEM, VMEM],
            input_output_aliases={0: 2, 1: 3}, name='store_first',
            cost_estimate=pl.CostEstimate(flops=10 ** 9, bytes_accessed=21 * 10 ** 6, transcendentals=0), **common,
        )(vm(k_mid), vm(v_mid), vm(kv_row), hbm(write_pos))
        v_new, _ = pl.pallas_call(
            functools.partial(store_second, jobs=((1, SPLIT, rows),)),
            out_shape=[full, held], in_specs=[VMEM, VMEM, ANY, ANY], out_specs=[ANY, VMEM],
            input_output_aliases={0: 1, 3: 0}, name='store_second',
            cost_estimate=pl.CostEstimate(flops=6 * 10 ** 8, bytes_accessed=13 * 10 ** 6, transcendentals=0), **common,
        )(vm(v_mid), vm(kv_row), hbm(write_pos), v_part)
        attn_out = pl.pallas_call(
            final,
            out_shape=jax.ShapeDtypeStruct((rows, w_out.shape[1]), BF16),
            in_specs=[VMEM] * 4,
            out_specs=VMEM,
            compiler_params=pltpu.CompilerParams(vmem_limit_bytes=4 * 2 ** 20),
            cost_estimate=pl.CostEstimate(flops=10 ** 6, bytes_accessed=2 ** 20, transcendentals=0),
            name='final',
        )(total, other, pair_own, pair_other)
        return attn_out, k_new.reshape(k_cache.shape), v_new.reshape(v_cache.shape)

    return jax.shard_map(one_step, mesh=mesh, in_specs=(row_spec, P(), P(), P(), P('sp', None), cache_spec, cache_spec, len_spec, len_spec), out_specs=(row_spec, cache_spec, cache_spec), check_vma=False)
```

```python
import functools

import jax
import jax.numpy as jnp
from jax import lax
from jax.experimental import pallas as pl
from jax.experimental.pallas import tpu as pltpu
from jax.sharding import PartitionSpec as P


F32, BF16 = jnp.float32, jnp.bfloat16
NEG_FLOOR = -1e30
GROUP = 8
FEED = (1, 1, 1, 2, 2, 2, 2)
CHUNKS = ((0, 48), (48, 64))
SPLIT = 48
EARLY = 1
ANY = pl.BlockSpec(memory_space=pl.ANY)
VMEM = pl.BlockSpec(memory_space=pltpu.VMEM)
SMEM = pl.BlockSpec(memory_space=pltpu.SMEM)
MESH = pl.DeviceIdType.MESH


def attend(hid_hbm, wq_hbm, wk_hbm, wv_hbm, wo_hbm, k_hbm, v_hbm, pos_hbm, len_hbm,
           total, k_buf, v_buf, kv_row,
           hid, wq, wkv, wo, q_all, pos, length, acc, ml, ml_in, parts, half, part3,
           sem_w, sem_s, sem_k, sem_v, send_q, recv_q, send_a, recv_a, send, recv):
    rows, span, dim = k_buf.shape
    heads = q_all.shape[0]
    groups = rows // GROUP
    wide = half.shape[1]
    mine = heads // 2
    i = lax.axis_index('sp')
    x, c = i // 2, i % 2
    peers = pair, across, far = 2 * x + 1 - c, 2 * (1 - x) + c, 2 * (1 - x) + 1 - c
    start = i * span
    barrier = pltpu.get_barrier_semaphore()

    own_cols = pl.ds(pl.multiple_of(c * wide, wide), wide)
    other_cols = pl.ds(pl.multiple_of((1 - c) * wide, wide), wide)

    def fetch(kind, g):
        part = pl.ds(g * GROUP, GROUP)
        if kind == 'o':
            cols = other_cols if g == 0 else own_cols
            return pltpu.make_async_copy(wo_hbm.at[:, cols], wo.at[:, cols], sem_w.at[2 if g == 0 else 3 + mine])
        if kind == 'k':
            return pltpu.make_async_copy(k_hbm.at[part], k_buf.at[part], sem_k.at[g])
        if g == groups - 1:
            part = pl.ds(g * GROUP + (kind == 'w') * GROUP // 2, GROUP // 2)
        return pltpu.make_async_copy(v_hbm.at[part], v_buf.at[part], sem_v.at[g + (kind == 'w')])

    def q_part(h):
        cols = pl.ds(pl.multiple_of((c * mine + h) * dim, dim), dim)
        return pltpu.make_async_copy(wq_hbm.at[:, cols], wq.at[h], sem_w.at[3 + h])

    def kv_part(hbm):
        return pltpu.make_async_copy(hbm, wkv, sem_w.at[1])

    def to(src, dst, sems, at, peer):
        return pltpu.make_async_remote_copy(src_ref=src, dst_ref=dst, send_sem=sems[0].at[at], recv_sem=sems[1].at[at],
                                            device_id={'sp': peer}, device_id_type=MESH)

    def heads_of(peer):
        return 2 * peer

    scal = [pltpu.make_async_copy(pos_hbm, pos, sem_s.at[0]), pltpu.make_async_copy(len_hbm, length, sem_s.at[1])]
    hidden = pltpu.make_async_copy(hid_hbm, hid, sem_w.at[0])
    hidden.start()

    @pl.when(c == 0)
    def _():
        kv_part(wk_hbm).start()

    @pl.when(c == 1)
    def _():
        kv_part(wv_hbm).start()

    for h in range(mine):
        q_part(h).start()
    for copy in scal:
        copy.start()
    for peer in peers:
        pl.semaphore_signal(barrier, inc=1, device_id={'sp': peer}, device_id_type=MESH)
    order = [('k', 0)]
    for g in range(1, groups):
        order += [('k', g), ('v', g - 1)]
    order += [('v', groups - 1), ('w', groups - 1)]
    started = []

    def begin(count):
        for item in order[len(started):len(started) + count]:
            started.append(item)
            fetch(*item).start()

    begin(FEED[0])
    for copy in scal:
        copy.wait()
    hidden.wait()
    kv_part(wk_hbm).wait()
    begin(FEED[1])
    kv_row[c] = jnp.dot(hid[...], wkv[...], preferred_element_type=F32).astype(BF16).astype(F32)
    for h in range(mine):
        q_part(h).wait()
        begin(FEED[2 + h])
        q_all[c * mine + h] = jnp.dot(hid[...], wq[h], preferred_element_type=F32).astype(BF16).astype(F32)
    for k in range(len(CHUNKS)):
        ml[k] = jnp.zeros(ml.shape[1:], F32)
    pl.semaphore_wait(barrier, 3)
    q_half = q_all.at[pl.ds(c * mine, mine)]
    swaps = [to(kv_row.at[c], kv_row.at[c], (send_q, recv_q), 0, pair), to(q_half, q_half, (send_q, recv_q), 1, pair)]
    for copy in swaps:
        copy.start()
    for copy in swaps:
        copy.wait()

    def score(g):
        base = g * GROUP
        here = slice(base, base + GROUP)
        k = [n for n, (r0, r1) in enumerate(CHUNKS) if r0 <= base < r1][0]
        q = jnp.swapaxes(q_all[:, here, :], 0, 1)
        fresh = jnp.sum(q * kv_row[0, here, :][:, None, :], axis=2, keepdims=True) * dim ** -0.5
        col = lax.broadcasted_iota(jnp.int32, (heads, span), 1) + start
        lane = lax.broadcasted_iota(jnp.int32, (heads, 128), 1)
        scores = []
        for j in range(GROUP):
            at, end = pos[base + j], length[base + j]
            s = lax.dot_general(q[j].astype(BF16), k_buf[base + j], (((1,), (1,)), ((), ())), preferred_element_type=F32)
            scores.append(jnp.where(jnp.logical_and(col < end, col != at), s * dim ** -0.5, -jnp.inf))
        probs, extra = [], []
        stats = ml[k]
        for j in range(GROUP):
            at, end = pos[base + j], length[base + j]
            owned = jnp.logical_and(jnp.logical_and(at >= start, at < start + span), at < end)
            s_new = jnp.where(owned, fresh[j], -jnp.inf)
            m = jnp.maximum(jnp.maximum(jnp.max(scores[j], axis=1, keepdims=True), s_new), NEG_FLOOR)
            p, p_new = jnp.exp(scores[j] - m), jnp.exp(s_new - m)
            spot = base + j - CHUNKS[k][0]
            stats = jnp.where(lane == spot, m, stats)
            stats = jnp.where(lane == 64 + spot, jnp.sum(p, axis=1, keepdims=True) + p_new, stats)
            probs.append(p.astype(BF16))
            extra.append(p_new)
        ml[k] = stats
        return probs, extra

    def blend(g, probs, extra):
        base = g * GROUP
        out = []
        for j in range(GROUP):
            if g == groups - 1 and j == GROUP // 2:
                fetch('w', g).wait()
                fetch('o', 0).start()
                fetch('o', 1).start()
            out.append(jnp.dot(probs[j], v_buf[base + j], preferred_element_type=F32) + extra[j] * kv_row[1, base + j:base + j + 1, :])
        acc[:, base:base + GROUP, :] = jnp.swapaxes(jnp.stack(out), 0, 1)

    def give_acc(g, n):
        rs = pl.ds(g * GROUP, GROUP)
        return to(acc.at[pl.ds(heads_of(peers[n]), 2), rs], parts.at[n, :, rs], (send_a, recv_a), (n, g), peers[n])

    def give(n, k):
        r0, r1 = CHUNKS[k]
        rs = pl.ds(r0, r1 - r0)
        sems = send, recv
        if n < 3:
            return to(ml.at[k], ml_in.at[n, k], sems, (n, k), peers[n])
        return to(half, part3, sems, (n, k), pair)

    def col_of(v, h):
        lane = lax.broadcasted_iota(jnp.int32, v.shape, 1)
        return jnp.sum(jnp.where(lane == h, v, 0.0), axis=1, keepdims=True)

    def combine(k):
        r0, r1 = CHUNKS[k]
        size = r1 - r0
        rs = slice(r0, r1)
        for q in range(3):
            give(q, k).wait()
        stats = []
        for v in (ml[k], ml_in[0, k], ml_in[1, k], ml_in[2, k]):
            t = v.T
            stats.append((t[:size], t[64:64 + size]))
        top = functools.reduce(jnp.maximum, [m for m, _ in stats])
        scale = [jnp.exp(m - top) for m, _ in stats]
        inv = 1.0 / functools.reduce(jnp.add, [l * e for (_, l), e in zip(stats, scale)])
        scale = [e * inv for e in scale]
        cols = [[col_of(e, heads_of(i) + j) for e in scale] for j in range(2)]
        for q in range(3):
            for g in range(r0 // GROUP, r1 // GROUP):
                give_acc(g, q).wait()
        o = []
        for j in range(2):
            part = acc[heads_of(i) + j, rs] * cols[j][0]
            for q in range(3):
                part += parts[q, j, rs] * cols[j][q + 1]
            o.append(part.astype(BF16))
        o = jnp.concatenate(o, axis=1)
        return o

    fetch('k', 0).wait()
    held = score(0)
    for g in range(groups):
        if g + 1 < groups:
            fetch('k', g + 1).wait()
        fetch('v', g).wait()
        begin(FEED[-1])
        following = score(g + 1) if g + 1 < groups else None
        blend(g, *held)
        held = following
        for k, (r0, r1) in enumerate(CHUNKS):
            if r1 == (g + 2) * GROUP:
                for n in (1, 2, 0):
                    give(n, k).start()
        for n in (1, 2, 0):
            give_acc(g, n).start()
    o = combine(0)
    early = CHUNKS[0][1]
    fetch('o', 0).wait()
    half[...] = jnp.dot(o, wo[:, other_cols], preferred_element_type=F32)
    give(3, 0).start()
    last = combine(1)
    fetch('o', 1).wait()
    own = jnp.dot(jnp.concatenate([o, last], axis=0), wo[:, own_cols], preferred_element_type=F32)
    total[early:rows] = own[early:]
    total[rows:] = jnp.dot(last, wo[:, other_cols], preferred_element_type=F32)
    give(3, 0).wait()
    total[:early] = own[:early] + part3[...]


def store(jobs, kv_row, pos_hbm, bufs, outs, pos, sem_p, sem_g, sem_w):
    span, dim = bufs[0].shape[1:]
    start = lax.axis_index('sp') * span
    sub = lax.broadcasted_iota(jnp.int32, (16, dim), 0)
    cuts = [(n, r) for n, r0, r1 in jobs for r in range(r0, r1, GROUP)]

    def place(b):
        at = pos[b] - start
        inside = jnp.logical_and(at >= 0, at < span)
        at = jnp.where(inside, at, 0)
        return at, inside, pl.ds(pl.multiple_of(at // 16 * 16, 16), 16)

    def patch(n, r):
        for b in range(r, r + GROUP):
            at, inside, win = place(b)
            hit = jnp.logical_and(sub == at % 16, inside)
            bufs[n][b, win, :] = jnp.where(hit, kv_row[n, b:b + 1, :], bufs[n][b, win, :].astype(F32)).astype(BF16)

    def put(n, r):
        part = pl.ds(r, GROUP)
        return pltpu.make_async_copy(bufs[n].at[part], outs[n].at[part], sem_g.at[n, r // GROUP])

    def windows(n, r, act):
        for b in range(r, r + GROUP):
            _, inside, win = place(b)

            @pl.when(inside)
            def _():
                act(pltpu.make_async_copy(bufs[n].at[b, win], outs[n].at[b, win], sem_w.at[b - cuts[0][1]]))

    ask = pltpu.make_async_copy(pos_hbm, pos, sem_p)
    ask.start()
    early, later = cuts[:EARLY], cuts[EARLY:]
    for cut in early:
        put(*cut).start()
    ask.wait()
    for cut in later:
        patch(*cut)
        put(*cut).start()
    for cut in early:
        put(*cut).wait()
        patch(*cut)
        windows(*cut, lambda copy: copy.start())
    for cut in later:
        put(*cut).wait()
    for cut in early:
        windows(*cut, lambda copy: copy.wait())


def store_first(k_in, v_in, kv_row, pos_hbm, k_out, v_out, k_buf, v_buf, *rest, jobs):
    store(jobs, kv_row, pos_hbm, (k_buf, v_buf), (k_out, v_out), *rest)


def store_second(v_in, kv_row, pos_hbm, v_old, v_out, v_buf, *rest, jobs):
    store(jobs, kv_row, pos_hbm, (v_buf, v_buf), (v_out, v_out), *rest)


def final(own, other, pair_own, pair_other, att, out, sem):
    rows, wide = out.shape[0], own.shape[1]
    early = CHUNKS[0][1]
    c = lax.axis_index('sp') % 2
    own_cols = pl.ds(pl.multiple_of(c * wide, wide), wide)
    other_cols = pl.ds(pl.multiple_of((1 - c) * wide, wide), wide)
    a, b = slice(early, rows), slice(rows, 2 * rows - early)
    out[:early, own_cols] = (own[:early] + other[:early]).astype(BF16)
    out[:early, other_cols] = (pair_own[:early] + pair_other[:early]).astype(BF16)
    first = pltpu.make_async_copy(out.at[:early], att.at[:early], sem.at[0])
    first.start()
    out[early:, own_cols] = ((own[a] + pair_own[b]) + (other[a] + pair_other[b])).astype(BF16)
    out[early:, other_cols] = ((own[b] + pair_own[a]) + (other[b] + pair_other[a])).astype(BF16)
    rest = pltpu.make_async_copy(out.at[early:], att.at[early:], sem.at[1])
    rest.start()
    first.wait()
    rest.wait()


def solution(mesh):
    row_spec = P(('rep', 'dp'), None)
    cache_spec = P(('rep', 'dp'), 'sp', None, None)
    len_spec = P(('rep', 'dp'))

    def one_step(hidden, w_query, w_key, w_value, w_out, k_cache, v_cache, write_pos, valid_len):
        rows, span, _, dim = k_cache.shape
        model = hidden.shape[1]
        heads = w_query.shape[1] // dim
        cache = (rows, span, dim)
        wide = w_out.shape[1] // 2
        pair = (2, rows, dim)
        chunks = len(CHUNKS)
        dma = pltpu.SemaphoreType.DMA
        hbm = lambda a: pltpu.with_memory_space_constraint(a, pltpu.HBM)
        vm = lambda a: pltpu.with_memory_space_constraint(a, pltpu.VMEM)
        total, k_mid, v_mid, kv_row = pl.pallas_call(
            attend,
            out_shape=[pltpu.VMEM((2 * rows - CHUNKS[0][1], wide), F32), pltpu.VMEM(cache, BF16), pltpu.VMEM(cache, BF16),
                       pltpu.VMEM((2, rows, dim), F32)],
            in_specs=[ANY] * 9,
            out_specs=[VMEM] * 4,
            scratch_shapes=[pltpu.VMEM((rows, model), BF16), pltpu.VMEM((heads // 2, model, dim), BF16),
                            pltpu.VMEM(w_key.shape, BF16), pltpu.VMEM(w_out.shape, BF16),
                            pltpu.VMEM((heads, rows, dim), F32),
                            pltpu.SMEM((rows,), jnp.int32), pltpu.SMEM((rows,), jnp.int32),
                            pltpu.VMEM((heads, rows, dim), F32), pltpu.VMEM((chunks, heads, 128), F32), pltpu.VMEM((3, chunks, heads, 128), F32),
                            pltpu.VMEM((3,) + pair, F32),
                            pltpu.VMEM((CHUNKS[0][1], wide), F32), pltpu.VMEM((CHUNKS[0][1], wide), F32),
                            dma((4 + heads // 2,)), dma((2,)), dma((rows // GROUP,)), dma((rows // GROUP + 1,)), dma((2,)), dma((2,)),
                            dma((3, rows // GROUP)), dma((3, rows // GROUP)), dma((4, chunks)), dma((4, chunks))],
            compiler_params=pltpu.CompilerParams(collective_id=0, has_side_effects=True, vmem_limit_bytes=12 * 2 ** 20),
            cost_estimate=pl.CostEstimate(flops=10 ** 9, bytes_accessed=46 * 10 ** 6, transcendentals=0),
            name='attend',
        )(*map(hbm, (hidden, w_query, w_key, w_value, w_out, k_cache.reshape(cache), v_cache.reshape(cache), write_pos, valid_len)))
        across = [(d, (d + 2) % 4) for d in range(4)]
        pairs = [(d, d ^ 1) for d in range(4)]
        other = lax.ppermute(total, 'sp', across)
        pair_own = lax.ppermute(total, 'sp', pairs)
        pair_other = lax.ppermute(other, 'sp', pairs)
        common = dict(
            scratch_shapes=[pltpu.SMEM((rows,), jnp.int32), dma, dma((2, rows // GROUP)), dma((EARLY * GROUP,))],
            compiler_params=pltpu.CompilerParams(vmem_limit_bytes=12 * 2 ** 20))
        full, held = pltpu.HBM(cache, BF16), pltpu.VMEM(cache, BF16)
        k_new, v_part, _, v_mid = pl.pallas_call(
            functools.partial(store_first, jobs=((0, 0, rows), (1, 0, SPLIT))),
            out_shape=[full, full, held, held], in_specs=[VMEM] * 3 + [ANY], out_specs=[ANY, ANY, VMEM, VMEM],
            input_output_aliases={0: 2, 1: 3}, name='store_first',
            cost_estimate=pl.CostEstimate(flops=10 ** 9, bytes_accessed=21 * 10 ** 6, transcendentals=0), **common,
        )(vm(k_mid), vm(v_mid), vm(kv_row), hbm(write_pos))
        v_new, _ = pl.pallas_call(
            functools.partial(store_second, jobs=((1, SPLIT, rows),)),
            out_shape=[full, held], in_specs=[VMEM, VMEM, ANY, ANY], out_specs=[ANY, VMEM],
            input_output_aliases={0: 1, 3: 0}, name='store_second',
            cost_estimate=pl.CostEstimate(flops=6 * 10 ** 8, bytes_accessed=13 * 10 ** 6, transcendentals=0), **common,
        )(vm(v_mid), vm(kv_row), hbm(write_pos), v_part)
        attn_out = pl.pallas_call(
            final,
            out_shape=pltpu.HBM((rows, w_out.shape[1]), BF16),
            in_specs=[VMEM] * 4,
            out_specs=ANY,
            scratch_shapes=[pltpu.VMEM((rows, w_out.shape[1]), BF16), dma((2,))],
            compiler_params=pltpu.CompilerParams(vmem_limit_bytes=4 * 2 ** 20),
            cost_estimate=pl.CostEstimate(flops=10 ** 6, bytes_accessed=2 ** 20, transcendentals=0),
            name='final',
        )(total, other, pair_own, pair_other)
        return attn_out, k_new.reshape(k_cache.shape), v_new.reshape(v_cache.shape)

    return jax.shard_map(one_step, mesh=mesh, in_specs=(row_spec, P(), P(), P(), P('sp', None), cache_spec, cache_spec, len_spec, len_spec), out_specs=(row_spec, cache_spec, cache_spec), check_vma=False)
```

```python
import functools

import jax
import jax.numpy as jnp
from jax import lax
from jax.experimental import pallas as pl
from jax.experimental.pallas import tpu as pltpu
from jax.sharding import PartitionSpec as P


F32, BF16 = jnp.float32, jnp.bfloat16
NEG_FLOOR = -1e30
GROUP = 8
FEED = (1, 1, 1, 2, 2, 2, 2)
CHUNKS = ((0, 48), (48, 64))
SPLIT = 56
LAST = 2
EARLY = 1
ANY = pl.BlockSpec(memory_space=pl.ANY)
VMEM = pl.BlockSpec(memory_space=pltpu.VMEM)
SMEM = pl.BlockSpec(memory_space=pltpu.SMEM)
MESH = pl.DeviceIdType.MESH


def attend(hid_hbm, wq_hbm, wk_hbm, wv_hbm, wo_hbm, k_hbm, v_hbm, pos_hbm, len_hbm,
           total, k_buf, v_buf, kv_row,
           hid, wq, wkv, wo, q_all, pos, length, acc, ml, ml_in, parts, half, part3,
           sem_w, sem_s, sem_k, sem_v, send_q, recv_q, send_a, recv_a, send, recv):
    rows, span, dim = k_buf.shape
    heads = q_all.shape[0]
    groups = rows // GROUP
    wide = half.shape[1]
    mine = heads // 2
    i = lax.axis_index('sp')
    x, c = i // 2, i % 2
    peers = pair, across, far = 2 * x + 1 - c, 2 * (1 - x) + c, 2 * (1 - x) + 1 - c
    start = i * span
    barrier = pltpu.get_barrier_semaphore()

    own_cols = pl.ds(pl.multiple_of(c * wide, wide), wide)
    other_cols = pl.ds(pl.multiple_of((1 - c) * wide, wide), wide)

    def fetch(kind, g):
        part = pl.ds(g * GROUP, GROUP)
        if kind == 'o':
            cols = other_cols if g == 0 else own_cols
            return pltpu.make_async_copy(wo_hbm.at[:, cols], wo.at[:, cols], sem_w.at[2 if g == 0 else 3 + mine])
        if kind == 'k':
            return pltpu.make_async_copy(k_hbm.at[part], k_buf.at[part], sem_k.at[g])
        if g == groups - 1:
            part = pl.ds(g * GROUP + (kind == 'w') * (GROUP - LAST), LAST if kind == 'w' else GROUP - LAST)
        return pltpu.make_async_copy(v_hbm.at[part], v_buf.at[part], sem_v.at[g + (kind == 'w')])

    def q_part(h):
        cols = pl.ds(pl.multiple_of((c * mine + h) * dim, dim), dim)
        return pltpu.make_async_copy(wq_hbm.at[:, cols], wq.at[h], sem_w.at[3 + h])

    def kv_part(hbm):
        return pltpu.make_async_copy(hbm, wkv, sem_w.at[1])

    def to(src, dst, sems, at, peer):
        return pltpu.make_async_remote_copy(src_ref=src, dst_ref=dst, send_sem=sems[0].at[at], recv_sem=sems[1].at[at],
                                            device_id={'sp': peer}, device_id_type=MESH)

    def heads_of(peer):
        return 2 * peer

    scal = [pltpu.make_async_copy(pos_hbm, pos, sem_s.at[0]), pltpu.make_async_copy(len_hbm, length, sem_s.at[1])]
    hidden = pltpu.make_async_copy(hid_hbm, hid, sem_w.at[0])
    hidden.start()

    @pl.when(c == 0)
    def _():
        kv_part(wk_hbm).start()

    @pl.when(c == 1)
    def _():
        kv_part(wv_hbm).start()

    for h in range(mine):
        q_part(h).start()
    for copy in scal:
        copy.start()
    for peer in peers:
        pl.semaphore_signal(barrier, inc=1, device_id={'sp': peer}, device_id_type=MESH)
    order = [('k', 0)]
    for g in range(1, groups):
        order += [('k', g), ('v', g - 1)]
    order += [('v', groups - 1), ('w', groups - 1)]
    started = []

    def begin(count):
        for item in order[len(started):len(started) + count]:
            started.append(item)
            fetch(*item).start()

    begin(FEED[0])
    for copy in scal:
        copy.wait()
    hidden.wait()
    kv_part(wk_hbm).wait()
    begin(FEED[1])
    kv_row[c] = jnp.dot(hid[...], wkv[...], preferred_element_type=F32).astype(BF16).astype(F32)
    for h in range(mine):
        q_part(h).wait()
        begin(FEED[2 + h])
        q_all[c * mine + h] = jnp.dot(hid[...], wq[h], preferred_element_type=F32).astype(BF16).astype(F32)
    for k in range(len(CHUNKS)):
        ml[k] = jnp.zeros(ml.shape[1:], F32)
    pl.semaphore_wait(barrier, 3)
    q_half = q_all.at[pl.ds(c * mine, mine)]
    swaps = [to(kv_row.at[c], kv_row.at[c], (send_q, recv_q), 0, pair), to(q_half, q_half, (send_q, recv_q), 1, pair)]
    for copy in swaps:
        copy.start()
    for copy in swaps:
        copy.wait()

    def score(g):
        base = g * GROUP
        here = slice(base, base + GROUP)
        k = [n for n, (r0, r1) in enumerate(CHUNKS) if r0 <= base < r1][0]
        q = jnp.swapaxes(q_all[:, here, :], 0, 1)
        fresh = jnp.sum(q * kv_row[0, here, :][:, None, :], axis=2, keepdims=True) * dim ** -0.5
        col = lax.broadcasted_iota(jnp.int32, (heads, span), 1) + start
        lane = lax.broadcasted_iota(jnp.int32, (heads, 128), 1)
        scores = []
        for j in range(GROUP):
            at, end = pos[base + j], length[base + j]
            s = lax.dot_general(q[j].astype(BF16), k_buf[base + j], (((1,), (1,)), ((), ())), preferred_element_type=F32)
            scores.append(jnp.where(jnp.logical_and(col < end, col != at), s * dim ** -0.5, -jnp.inf))
        probs, extra = [], []
        stats = ml[k]
        for j in range(GROUP):
            at, end = pos[base + j], length[base + j]
            owned = jnp.logical_and(jnp.logical_and(at >= start, at < start + span), at < end)
            s_new = jnp.where(owned, fresh[j], -jnp.inf)
            m = jnp.maximum(jnp.maximum(jnp.max(scores[j], axis=1, keepdims=True), s_new), NEG_FLOOR)
            p, p_new = jnp.exp(scores[j] - m), jnp.exp(s_new - m)
            spot = base + j - CHUNKS[k][0]
            stats = jnp.where(lane == spot, m, stats)
            stats = jnp.where(lane == 64 + spot, jnp.sum(p, axis=1, keepdims=True) + p_new, stats)
            probs.append(p.astype(BF16))
            extra.append(p_new)
        ml[k] = stats
        return probs, extra

    def blend(g, probs, extra):
        base = g * GROUP
        out = []
        for j in range(GROUP):
            if g == groups - 1 and j == GROUP - LAST:
                fetch('o', 0).start()
                fetch('w', g).wait()
                fetch('o', 1).start()
            out.append(jnp.dot(probs[j], v_buf[base + j], preferred_element_type=F32) + extra[j] * kv_row[1, base + j:base + j + 1, :])
        acc[:, base:base + GROUP, :] = jnp.swapaxes(jnp.stack(out), 0, 1)

    def give_acc(g, n):
        rs = pl.ds(g * GROUP, GROUP)
        return to(acc.at[pl.ds(heads_of(peers[n]), 2), rs], parts.at[n, :, rs], (send_a, recv_a), (n, g), peers[n])

    def give(n, k):
        r0, r1 = CHUNKS[k]
        rs = pl.ds(r0, r1 - r0)
        sems = send, recv
        if n < 3:
            return to(ml.at[k], ml_in.at[n, k], sems, (n, k), peers[n])
        return to(half, part3, sems, (n, k), pair)

    def col_of(v, h):
        lane = lax.broadcasted_iota(jnp.int32, v.shape, 1)
        return jnp.sum(jnp.where(lane == h, v, 0.0), axis=1, keepdims=True)

    def combine(k):
        r0, r1 = CHUNKS[k]
        size = r1 - r0
        rs = slice(r0, r1)
        for q in range(3):
            give(q, k).wait()
        stats = []
        for v in (ml[k], ml_in[0, k], ml_in[1, k], ml_in[2, k]):
            t = v.T
            stats.append((t[:size], t[64:64 + size]))
        top = functools.reduce(jnp.maximum, [m for m, _ in stats])
        scale = [jnp.exp(m - top) for m, _ in stats]
        inv = 1.0 / functools.reduce(jnp.add, [l * e for (_, l), e in zip(stats, scale)])
        scale = [e * inv for e in scale]
        cols = [[col_of(e, heads_of(i) + j) for e in scale] for j in range(2)]
        o = [acc[heads_of(i) + j, rs] * cols[j][0] for j in range(2)]
        for q in (0, 1, 2):
            for g in range(r0 // GROUP, r1 // GROUP):
                give_acc(g, q).wait()
            o = [o[j] + parts[q, j, rs] * cols[j][q + 1] for j in range(2)]
        return jnp.concatenate([part.astype(BF16) for part in o], axis=1)

    fetch('k', 0).wait()
    held = score(0)
    for g in range(groups):
        if g + 1 < groups:
            fetch('k', g + 1).wait()
        fetch('v', g).wait()
        begin(FEED[-1])
        following = score(g + 1) if g + 1 < groups else None
        blend(g, *held)
        held = following
        for k, (r0, r1) in enumerate(CHUNKS):
            if r1 == (g + 2) * GROUP:
                for n in (1, 2, 0):
                    give(n, k).start()
        for n in (1, 2, 0):
            give_acc(g, n).start()
    o = combine(0)
    early = CHUNKS[0][1]
    fetch('o', 0).wait()
    half[...] = jnp.dot(o, wo[:, other_cols], preferred_element_type=F32)
    give(3, 0).start()
    last = combine(1)
    fetch('o', 1).wait()
    own = jnp.dot(jnp.concatenate([o, last], axis=0), wo[:, own_cols], preferred_element_type=F32)
    total[early:rows] = own[early:]
    total[rows:] = jnp.dot(last, wo[:, other_cols], preferred_element_type=F32)
    give(3, 0).wait()
    total[:early] = own[:early] + part3[...]


def store(jobs, kv_row, pos_hbm, bufs, outs, pos, sem_p, sem_g, sem_w):
    span, dim = bufs[0].shape[1:]
    start = lax.axis_index('sp') * span
    sub = lax.broadcasted_iota(jnp.int32, (16, dim), 0)
    cuts = [(n, r) for n, r0, r1 in jobs for r in range(r0, r1, GROUP)]

    def place(b):
        at = pos[b] - start
        inside = jnp.logical_and(at >= 0, at < span)
        at = jnp.where(inside, at, 0)
        return at, inside, pl.ds(pl.multiple_of(at // 16 * 16, 16), 16)

    def patch(n, r):
        for b in range(r, r + GROUP):
            at, inside, win = place(b)
            hit = jnp.logical_and(sub == at % 16, inside)
            bufs[n][b, win, :] = jnp.where(hit, kv_row[n, b:b + 1, :], bufs[n][b, win, :].astype(F32)).astype(BF16)

    def put(n, r):
        part = pl.ds(r, GROUP)
        return pltpu.make_async_copy(bufs[n].at[part], outs[n].at[part], sem_g.at[n, r // GROUP])

    def windows(n, r, act):
        for b in range(r, r + GROUP):
            _, inside, win = place(b)

            @pl.when(inside)
            def _():
                act(pltpu.make_async_copy(bufs[n].at[b, win], outs[n].at[b, win], sem_w.at[b - cuts[0][1]]))

    ask = pltpu.make_async_copy(pos_hbm, pos, sem_p)
    ask.start()
    early, later = cuts[:EARLY], cuts[EARLY:]
    for cut in early:
        put(*cut).start()
    ask.wait()
    for cut in later:
        patch(*cut)
        put(*cut).start()
    for r in range(jobs[-1][2], bufs[1].shape[0], GROUP):
        patch(1, r)
    for cut in early:
        put(*cut).wait()
        patch(*cut)
        windows(*cut, lambda copy: copy.start())
    for cut in later:
        put(*cut).wait()
    for cut in early:
        windows(*cut, lambda copy: copy.wait())


def store_first(k_in, v_in, kv_row, pos_hbm, k_out, v_out, k_buf, v_buf, *rest, jobs):
    store(jobs, kv_row, pos_hbm, (k_buf, v_buf), (k_out, v_out), *rest)


def store_second(v_in, v_old, v_out, v_buf, sem):
    copies = [pltpu.make_async_copy(v_buf.at[pl.ds(r, GROUP)], v_out.at[pl.ds(r, GROUP)], sem.at[n])
              for n, r in enumerate(range(SPLIT, v_buf.shape[0], GROUP))]
    for copy in copies:
        copy.start()
    for copy in copies:
        copy.wait()


def final(own, other, pair_own, pair_other, att, out, sem):
    rows, wide = out.shape[0], own.shape[1]
    early = CHUNKS[0][1]
    c = lax.axis_index('sp') % 2
    own_cols = pl.ds(pl.multiple_of(c * wide, wide), wide)
    other_cols = pl.ds(pl.multiple_of((1 - c) * wide, wide), wide)
    a, b = slice(early, rows), slice(rows, 2 * rows - early)
    out[:early, own_cols] = (own[:early] + other[:early]).astype(BF16)
    out[:early, other_cols] = (pair_own[:early] + pair_other[:early]).astype(BF16)
    first = pltpu.make_async_copy(out.at[:early], att.at[:early], sem.at[0])
    first.start()
    out[early:, own_cols] = ((own[a] + pair_own[b]) + (other[a] + pair_other[b])).astype(BF16)
    out[early:, other_cols] = ((own[b] + pair_own[a]) + (other[b] + pair_other[a])).astype(BF16)
    rest = pltpu.make_async_copy(out.at[early:], att.at[early:], sem.at[1])
    rest.start()
    first.wait()
    rest.wait()


def solution(mesh):
    row_spec = P(('rep', 'dp'), None)
    cache_spec = P(('rep', 'dp'), 'sp', None, None)
    len_spec = P(('rep', 'dp'))

    def one_step(hidden, w_query, w_key, w_value, w_out, k_cache, v_cache, write_pos, valid_len):
        rows, span, _, dim = k_cache.shape
        model = hidden.shape[1]
        heads = w_query.shape[1] // dim
        cache = (rows, span, dim)
        wide = w_out.shape[1] // 2
        pair = (2, rows, dim)
        chunks = len(CHUNKS)
        dma = pltpu.SemaphoreType.DMA
        hbm = lambda a: pltpu.with_memory_space_constraint(a, pltpu.HBM)
        vm = lambda a: pltpu.with_memory_space_constraint(a, pltpu.VMEM)
        total, k_mid, v_mid, kv_row = pl.pallas_call(
            attend,
            out_shape=[pltpu.VMEM((2 * rows - CHUNKS[0][1], wide), F32), pltpu.VMEM(cache, BF16), pltpu.VMEM(cache, BF16),
                       pltpu.VMEM((2, rows, dim), F32)],
            in_specs=[ANY] * 9,
            out_specs=[VMEM] * 4,
            scratch_shapes=[pltpu.VMEM((rows, model), BF16), pltpu.VMEM((heads // 2, model, dim), BF16),
                            pltpu.VMEM(w_key.shape, BF16), pltpu.VMEM(w_out.shape, BF16),
                            pltpu.VMEM((heads, rows, dim), F32),
                            pltpu.SMEM((rows,), jnp.int32), pltpu.SMEM((rows,), jnp.int32),
                            pltpu.VMEM((heads, rows, dim), F32), pltpu.VMEM((chunks, heads, 128), F32), pltpu.VMEM((3, chunks, heads, 128), F32),
                            pltpu.VMEM((3,) + pair, F32),
                            pltpu.VMEM((CHUNKS[0][1], wide), F32), pltpu.VMEM((CHUNKS[0][1], wide), F32),
                            dma((4 + heads // 2,)), dma((2,)), dma((rows // GROUP,)), dma((rows // GROUP + 1,)), dma((2,)), dma((2,)),
                            dma((3, rows // GROUP)), dma((3, rows // GROUP)), dma((4, chunks)), dma((4, chunks))],
            compiler_params=pltpu.CompilerParams(collective_id=0, has_side_effects=True, vmem_limit_bytes=12 * 2 ** 20),
            cost_estimate=pl.CostEstimate(flops=10 ** 9, bytes_accessed=46 * 10 ** 6, transcendentals=0),
            name='attend',
        )(*map(hbm, (hidden, w_query, w_key, w_value, w_out, k_cache.reshape(cache), v_cache.reshape(cache), write_pos, valid_len)))
        across = [(d, (d + 2) % 4) for d in range(4)]
        pairs = [(d, d ^ 1) for d in range(4)]
        other = lax.ppermute(total, 'sp', across)
        pair_own = lax.ppermute(total, 'sp', pairs)
        pair_other = lax.ppermute(other, 'sp', pairs)
        common = dict(
            scratch_shapes=[pltpu.SMEM((rows,), jnp.int32), dma, dma((2, rows // GROUP)), dma((EARLY * GROUP,))],
            compiler_params=pltpu.CompilerParams(vmem_limit_bytes=12 * 2 ** 20))
        full, held = pltpu.HBM(cache, BF16), pltpu.VMEM(cache, BF16)
        k_new, v_part, _, v_mid = pl.pallas_call(
            functools.partial(store_first, jobs=((0, 0, rows), (1, 0, SPLIT))),
            out_shape=[full, full, held, held], in_specs=[VMEM] * 3 + [ANY], out_specs=[ANY, ANY, VMEM, VMEM],
            input_output_aliases={0: 2, 1: 3}, name='store_first',
            cost_estimate=pl.CostEstimate(flops=10 ** 9, bytes_accessed=21 * 10 ** 6, transcendentals=0), **common,
        )(vm(k_mid), vm(v_mid), vm(kv_row), hbm(write_pos))
        v_new, _ = pl.pallas_call(
            store_second,
            out_shape=[full, held], in_specs=[VMEM, ANY], out_specs=[ANY, VMEM],
            input_output_aliases={0: 1, 1: 0}, name='store_second', scratch_shapes=[dma(((rows - SPLIT) // GROUP,))],
            compiler_params=common['compiler_params'],
            cost_estimate=pl.CostEstimate(flops=6 * 10 ** 8, bytes_accessed=13 * 10 ** 6, transcendentals=0),
        )(vm(v_mid), v_part)
        attn_out = pl.pallas_call(
            final,
            out_shape=pltpu.HBM((rows, w_out.shape[1]), BF16),
            in_specs=[VMEM] * 4,
            out_specs=ANY,
            scratch_shapes=[pltpu.VMEM((rows, w_out.shape[1]), BF16), dma((2,))],
            compiler_params=pltpu.CompilerParams(vmem_limit_bytes=4 * 2 ** 20),
            cost_estimate=pl.CostEstimate(flops=10 ** 6, bytes_accessed=2 ** 20, transcendentals=0),
            name='final',
        )(total, other, pair_own, pair_other)
        return attn_out, k_new.reshape(k_cache.shape), v_new.reshape(v_cache.shape)

    return jax.shard_map(one_step, mesh=mesh, in_specs=(row_spec, P(), P(), P(), P('sp', None), cache_spec, cache_spec, len_spec, len_spec), out_specs=(row_spec, cache_spec, cache_spec), check_vma=False)
```

```python
import functools

import jax
import jax.numpy as jnp
from jax import lax
from jax.experimental import pallas as pl
from jax.experimental.pallas import tpu as pltpu
from jax.sharding import PartitionSpec as P


F32, BF16 = jnp.float32, jnp.bfloat16
NEG_FLOOR = float(jnp.finfo(jnp.float32).min)
GROUP = 8
FEED = (1, 1, 1, 2, 2, 2, 2)
CHUNKS = ((0, 48), (48, 64))
SPLIT = 56
LAST = 2
EARLY = 1
ANY = pl.BlockSpec(memory_space=pl.ANY)
VMEM = pl.BlockSpec(memory_space=pltpu.VMEM)
SMEM = pl.BlockSpec(memory_space=pltpu.SMEM)
MESH = pl.DeviceIdType.MESH


def attend(hid_hbm, wq_hbm, wk_hbm, wv_hbm, wo_hbm, k_hbm, v_hbm, pos_hbm, len_hbm,
           total, k_buf, v_buf, kv_row,
           hid, wq, wkv, wo, q_all, pos, length, acc, ml, ml_in, parts, half, part3,
           sem_w, sem_s, sem_k, sem_v, send_q, recv_q, send_a, recv_a, send, recv):
    rows, span, dim = k_buf.shape
    heads = q_all.shape[0]
    groups = rows // GROUP
    wide = half.shape[1]
    mine = heads // 2
    i = lax.axis_index('sp')
    x, c = i // 2, i % 2
    peers = pair, across, far = 2 * x + 1 - c, 2 * (1 - x) + c, 2 * (1 - x) + 1 - c
    start = i * span
    barrier = pltpu.get_barrier_semaphore()

    own_cols = pl.ds(pl.multiple_of(c * wide, wide), wide)
    other_cols = pl.ds(pl.multiple_of((1 - c) * wide, wide), wide)

    def fetch(kind, g):
        part = pl.ds(g * GROUP, GROUP)
        if kind == 'o':
            cols = other_cols if g == 0 else own_cols
            return pltpu.make_async_copy(wo_hbm.at[:, cols], wo.at[:, cols], sem_w.at[2 if g == 0 else 3 + mine])
        if kind == 'k':
            return pltpu.make_async_copy(k_hbm.at[part], k_buf.at[part], sem_k.at[g])
        if g == groups - 1:
            part = pl.ds(g * GROUP + (kind == 'w') * (GROUP - LAST), LAST if kind == 'w' else GROUP - LAST)
        return pltpu.make_async_copy(v_hbm.at[part], v_buf.at[part], sem_v.at[g + (kind == 'w')])

    def q_part(h):
        cols = pl.ds(pl.multiple_of((c * mine + h) * dim, dim), dim)
        return pltpu.make_async_copy(wq_hbm.at[:, cols], wq.at[h], sem_w.at[3 + h])

    def kv_part(hbm):
        return pltpu.make_async_copy(hbm, wkv, sem_w.at[1])

    def to(src, dst, sems, at, peer):
        return pltpu.make_async_remote_copy(src_ref=src, dst_ref=dst, send_sem=sems[0].at[at], recv_sem=sems[1].at[at],
                                            device_id={'sp': peer}, device_id_type=MESH)

    def heads_of(peer):
        return 2 * peer

    scal = [pltpu.make_async_copy(pos_hbm, pos, sem_s.at[0]), pltpu.make_async_copy(len_hbm, length, sem_s.at[1])]
    hidden = pltpu.make_async_copy(hid_hbm, hid, sem_w.at[0])
    hidden.start()

    @pl.when(c == 0)
    def _():
        kv_part(wk_hbm).start()

    @pl.when(c == 1)
    def _():
        kv_part(wv_hbm).start()

    for h in range(mine):
        q_part(h).start()
    for copy in scal:
        copy.start()
    for peer in peers:
        pl.semaphore_signal(barrier, inc=1, device_id={'sp': peer}, device_id_type=MESH)
    order = [('k', 0)]
    for g in range(1, groups):
        order += [('k', g), ('v', g - 1)]
    order += [('v', groups - 1), ('w', groups - 1)]
    started = []

    def begin(count):
        for item in order[len(started):len(started) + count]:
            started.append(item)
            fetch(*item).start()

    begin(FEED[0])
    for copy in scal:
        copy.wait()
    hidden.wait()
    kv_part(wk_hbm).wait()
    begin(FEED[1])
    kv_row[c] = jnp.dot(hid[...], wkv[...], preferred_element_type=F32).astype(BF16).astype(F32)
    for h in range(mine):
        q_part(h).wait()
        begin(FEED[2 + h])
        q_all[c * mine + h] = jnp.dot(hid[...], wq[h], preferred_element_type=F32).astype(BF16).astype(F32)
    for k in range(len(CHUNKS)):
        ml[k] = jnp.zeros(ml.shape[1:], F32)
    pl.semaphore_wait(barrier, 3)
    q_half = q_all.at[pl.ds(c * mine, mine)]
    swaps = [to(kv_row.at[c], kv_row.at[c], (send_q, recv_q), 0, pair), to(q_half, q_half, (send_q, recv_q), 1, pair)]
    for copy in swaps:
        copy.start()
    for copy in swaps:
        copy.wait()

    def score(g):
        base = g * GROUP
        here = slice(base, base + GROUP)
        k = [n for n, (r0, r1) in enumerate(CHUNKS) if r0 <= base < r1][0]
        q = jnp.swapaxes(q_all[:, here, :], 0, 1)
        fresh = jnp.sum(q * kv_row[0, here, :][:, None, :], axis=2, keepdims=True) * dim ** -0.5
        col = lax.broadcasted_iota(jnp.int32, (heads, span), 1) + start
        lane = lax.broadcasted_iota(jnp.int32, (heads, 128), 1)
        scores = []
        for j in range(GROUP):
            at, end = pos[base + j], length[base + j]
            s = lax.dot_general(q[j].astype(BF16), k_buf[base + j], (((1,), (1,)), ((), ())), preferred_element_type=F32)
            scores.append(jnp.where(jnp.logical_and(col < end, col != at), s * dim ** -0.5, -jnp.inf))
        probs, extra = [], []
        stats = ml[k]
        for j in range(GROUP):
            at, end = pos[base + j], length[base + j]
            owned = jnp.logical_and(jnp.logical_and(at >= start, at < start + span), at < end)
            s_new = jnp.where(owned, fresh[j], -jnp.inf)
            m = jnp.maximum(jnp.maximum(jnp.max(scores[j], axis=1, keepdims=True), s_new), NEG_FLOOR)
            p, p_new = jnp.exp(scores[j] - m), jnp.exp(s_new - m)
            spot = base + j - CHUNKS[k][0]
            stats = jnp.where(lane == spot, m, stats)
            stats = jnp.where(lane == 64 + spot, jnp.sum(p, axis=1, keepdims=True) + p_new, stats)
            probs.append(p.astype(BF16))
            extra.append(p_new)
        ml[k] = stats
        return probs, extra

    def blend(g, probs, extra):
        base = g * GROUP
        out = []
        for j in range(GROUP):
            if g == groups - 1 and j == GROUP - LAST:
                fetch('o', 0).start()
                fetch('w', g).wait()
                fetch('o', 1).start()
            out.append(jnp.dot(probs[j], v_buf[base + j], preferred_element_type=F32) + extra[j] * kv_row[1, base + j:base + j + 1, :])
        acc[:, base:base + GROUP, :] = jnp.swapaxes(jnp.stack(out), 0, 1)

    def give_acc(g, n):
        rs = pl.ds(g * GROUP, GROUP)
        return to(acc.at[pl.ds(heads_of(peers[n]), 2), rs], parts.at[n, :, rs], (send_a, recv_a), (n, g), peers[n])

    def give(n, k):
        r0, r1 = CHUNKS[k]
        rs = pl.ds(r0, r1 - r0)
        sems = send, recv
        if n < 3:
            return to(ml.at[k], ml_in.at[n, k], sems, (n, k), peers[n])
        return to(half, part3, sems, (n, k), pair)

    def col_of(v, h):
        lane = lax.broadcasted_iota(jnp.int32, v.shape, 1)
        return jnp.sum(jnp.where(lane == h, v, 0.0), axis=1, keepdims=True)

    def combine(k):
        r0, r1 = CHUNKS[k]
        size = r1 - r0
        rs = slice(r0, r1)
        for q in range(3):
            give(q, k).wait()
        stats = []
        for v in (ml[k], ml_in[0, k], ml_in[1, k], ml_in[2, k]):
            t = v.T
            stats.append((t[:size], t[64:64 + size]))
        top = functools.reduce(jnp.maximum, [m for m, _ in stats])
        scale = [jnp.exp(m - top) for m, _ in stats]
        inv = 1.0 / functools.reduce(jnp.add, [l * e for (_, l), e in zip(stats, scale)])
        scale = [e * inv for e in scale]
        cols = [[col_of(e, heads_of(i) + j) for e in scale] for j in range(2)]
        o = [acc[heads_of(i) + j, rs] * cols[j][0] for j in range(2)]
        for q in (0, 1, 2):
            for g in range(r0 // GROUP, r1 // GROUP):
                give_acc(g, q).wait()
            o = [o[j] + parts[q, j, rs] * cols[j][q + 1] for j in range(2)]
        return jnp.concatenate([part.astype(BF16) for part in o], axis=1)

    fetch('k', 0).wait()
    held = score(0)
    for g in range(groups):
        if g + 1 < groups:
            fetch('k', g + 1).wait()
        fetch('v', g).wait()
        begin(FEED[-1])
        following = score(g + 1) if g + 1 < groups else None
        blend(g, *held)
        held = following
        for k, (r0, r1) in enumerate(CHUNKS):
            if r1 == (g + 2) * GROUP:
                for n in (1, 2, 0):
                    give(n, k).start()
        for n in (1, 2, 0):
            give_acc(g, n).start()
    o = combine(0)
    early = CHUNKS[0][1]
    fetch('o', 0).wait()
    half[...] = jnp.dot(o, wo[:, other_cols], preferred_element_type=F32)
    give(3, 0).start()
    fetch('o', 1).wait()
    total[:early] = jnp.dot(o, wo[:, own_cols], preferred_element_type=F32)
    o = combine(1)
    total[early:rows] = jnp.dot(o, wo[:, own_cols], preferred_element_type=F32)
    total[rows:] = jnp.dot(o, wo[:, other_cols], preferred_element_type=F32)
    give(3, 0).wait()
    total[:early] += part3[...]


def store(jobs, kv_row, pos_hbm, bufs, outs, pos, sem_p, sem_g, sem_w):
    span, dim = bufs[0].shape[1:]
    start = lax.axis_index('sp') * span
    sub = lax.broadcasted_iota(jnp.int32, (16, dim), 0)
    cuts = [(n, r) for n, r0, r1 in jobs for r in range(r0, r1, GROUP)]

    def place(b):
        at = pos[b] - start
        inside = jnp.logical_and(at >= 0, at < span)
        at = jnp.where(inside, at, 0)
        return at, inside, pl.ds(pl.multiple_of(at // 16 * 16, 16), 16)

    def patch(n, r):
        for b in range(r, r + GROUP):
            at, inside, win = place(b)
            hit = jnp.logical_and(sub == at % 16, inside)
            bufs[n][b, win, :] = jnp.where(hit, kv_row[n, b:b + 1, :], bufs[n][b, win, :].astype(F32)).astype(BF16)

    def put(n, r):
        part = pl.ds(r, GROUP)
        return pltpu.make_async_copy(bufs[n].at[part], outs[n].at[part], sem_g.at[n, r // GROUP])

    def windows(n, r, act):
        for b in range(r, r + GROUP):
            _, inside, win = place(b)

            @pl.when(inside)
            def _():
                act(pltpu.make_async_copy(bufs[n].at[b, win], outs[n].at[b, win], sem_w.at[b - cuts[0][1]]))

    ask = pltpu.make_async_copy(pos_hbm, pos, sem_p)
    ask.start()
    early, later = cuts[:EARLY], cuts[EARLY:]
    for cut in early:
        put(*cut).start()
    ask.wait()
    for cut in later:
        patch(*cut)
        put(*cut).start()
    for r in range(jobs[-1][2], bufs[1].shape[0], GROUP):
        patch(1, r)
    for cut in early:
        put(*cut).wait()
        patch(*cut)
        windows(*cut, lambda copy: copy.start())
    for cut in later:
        put(*cut).wait()
    for cut in early:
        windows(*cut, lambda copy: copy.wait())


def store_first(k_in, v_in, kv_row, pos_hbm, k_out, v_out, k_buf, v_buf, *rest, jobs):
    store(jobs, kv_row, pos_hbm, (k_buf, v_buf), (k_out, v_out), *rest)


def store_second(v_in, v_old, v_out, v_buf, sem):
    copies = [pltpu.make_async_copy(v_buf.at[pl.ds(r, GROUP)], v_out.at[pl.ds(r, GROUP)], sem.at[n])
              for n, r in enumerate(range(SPLIT, v_buf.shape[0], GROUP))]
    for copy in copies:
        copy.start()
    for copy in copies:
        copy.wait()


def final(own, other, pair_own, pair_other, att, out, sem):
    rows, wide = out.shape[0], own.shape[1]
    early = CHUNKS[0][1]
    c = lax.axis_index('sp') % 2
    own_cols = pl.ds(pl.multiple_of(c * wide, wide), wide)
    other_cols = pl.ds(pl.multiple_of((1 - c) * wide, wide), wide)
    a, b = slice(early, rows), slice(rows, 2 * rows - early)
    out[:early, own_cols] = (own[:early] + other[:early]).astype(BF16)
    out[:early, other_cols] = (pair_own[:early] + pair_other[:early]).astype(BF16)
    first = pltpu.make_async_copy(out.at[:early], att.at[:early], sem.at[0])
    first.start()
    out[early:, own_cols] = ((own[a] + pair_own[b]) + (other[a] + pair_other[b])).astype(BF16)
    out[early:, other_cols] = ((own[b] + pair_own[a]) + (other[b] + pair_other[a])).astype(BF16)
    rest = pltpu.make_async_copy(out.at[early:], att.at[early:], sem.at[1])
    rest.start()
    first.wait()
    rest.wait()


def solution(mesh):
    row_spec = P(('rep', 'dp'), None)
    cache_spec = P(('rep', 'dp'), 'sp', None, None)
    len_spec = P(('rep', 'dp'))

    def one_step(hidden, w_query, w_key, w_value, w_out, k_cache, v_cache, write_pos, valid_len):
        rows, span, _, dim = k_cache.shape
        model = hidden.shape[1]
        heads = w_query.shape[1] // dim
        cache = (rows, span, dim)
        wide = w_out.shape[1] // 2
        pair = (2, rows, dim)
        chunks = len(CHUNKS)
        dma = pltpu.SemaphoreType.DMA
        hbm = lambda a: pltpu.with_memory_space_constraint(a, pltpu.HBM)
        vm = lambda a: pltpu.with_memory_space_constraint(a, pltpu.VMEM)
        total, k_mid, v_mid, kv_row = pl.pallas_call(
            attend,
            out_shape=[pltpu.VMEM((2 * rows - CHUNKS[0][1], wide), F32), pltpu.VMEM(cache, BF16), pltpu.VMEM(cache, BF16),
                       pltpu.VMEM((2, rows, dim), F32)],
            in_specs=[ANY] * 9,
            out_specs=[VMEM] * 4,
            scratch_shapes=[pltpu.VMEM((rows, model), BF16), pltpu.VMEM((heads // 2, model, dim), BF16),
                            pltpu.VMEM(w_key.shape, BF16), pltpu.VMEM(w_out.shape, BF16),
                            pltpu.VMEM((heads, rows, dim), F32),
                            pltpu.SMEM((rows,), jnp.int32), pltpu.SMEM((rows,), jnp.int32),
                            pltpu.VMEM((heads, rows, dim), F32), pltpu.VMEM((chunks, heads, 128), F32), pltpu.VMEM((3, chunks, heads, 128), F32),
                            pltpu.VMEM((3,) + pair, F32),
                            pltpu.VMEM((CHUNKS[0][1], wide), F32), pltpu.VMEM((CHUNKS[0][1], wide), F32),
                            dma((4 + heads // 2,)), dma((2,)), dma((rows // GROUP,)), dma((rows // GROUP + 1,)), dma((2,)), dma((2,)),
                            dma((3, rows // GROUP)), dma((3, rows // GROUP)), dma((4, chunks)), dma((4, chunks))],
            compiler_params=pltpu.CompilerParams(collective_id=0, has_side_effects=True, vmem_limit_bytes=12 * 2 ** 20),
            cost_estimate=pl.CostEstimate(flops=10 ** 9, bytes_accessed=46 * 10 ** 6, transcendentals=0),
            name='attend',
        )(*map(hbm, (hidden, w_query, w_key, w_value, w_out, k_cache.reshape(cache), v_cache.reshape(cache), write_pos, valid_len)))
        across = [(d, (d + 2) % 4) for d in range(4)]
        pairs = [(d, d ^ 1) for d in range(4)]
        other = lax.ppermute(total, 'sp', across)
        pair_own = lax.ppermute(total, 'sp', pairs)
        pair_other = lax.ppermute(other, 'sp', pairs)
        common = dict(
            scratch_shapes=[pltpu.SMEM((rows,), jnp.int32), dma, dma((2, rows // GROUP)), dma((EARLY * GROUP,))],
            compiler_params=pltpu.CompilerParams(vmem_limit_bytes=12 * 2 ** 20))
        full, held = pltpu.HBM(cache, BF16), pltpu.VMEM(cache, BF16)
        k_new, v_part, _, v_mid = pl.pallas_call(
            functools.partial(store_first, jobs=((0, 0, rows), (1, 0, SPLIT))),
            out_shape=[full, full, held, held], in_specs=[VMEM] * 3 + [ANY], out_specs=[ANY, ANY, VMEM, VMEM],
            input_output_aliases={0: 2, 1: 3}, name='store_first',
            cost_estimate=pl.CostEstimate(flops=10 ** 9, bytes_accessed=21 * 10 ** 6, transcendentals=0), **common,
        )(vm(k_mid), vm(v_mid), vm(kv_row), hbm(write_pos))
        v_new, _ = pl.pallas_call(
            store_second,
            out_shape=[full, held], in_specs=[VMEM, ANY], out_specs=[ANY, VMEM],
            input_output_aliases={0: 1, 1: 0}, name='store_second', scratch_shapes=[dma(((rows - SPLIT) // GROUP,))],
            compiler_params=common['compiler_params'],
            cost_estimate=pl.CostEstimate(flops=6 * 10 ** 8, bytes_accessed=13 * 10 ** 6, transcendentals=0),
        )(vm(v_mid), v_part)
        attn_out = pl.pallas_call(
            final,
            out_shape=pltpu.HBM((rows, w_out.shape[1]), BF16),
            in_specs=[VMEM] * 4,
            out_specs=ANY,
            scratch_shapes=[pltpu.VMEM((rows, w_out.shape[1]), BF16), dma((2,))],
            compiler_params=pltpu.CompilerParams(vmem_limit_bytes=4 * 2 ** 20),
            cost_estimate=pl.CostEstimate(flops=10 ** 6, bytes_accessed=2 ** 20, transcendentals=0),
            name='final',
        )(total, other, pair_own, pair_other)
        return attn_out, k_new.reshape(k_cache.shape), v_new.reshape(v_cache.shape)

    return jax.shard_map(one_step, mesh=mesh, in_specs=(row_spec, P(), P(), P(), P('sp', None), cache_spec, cache_spec, len_spec, len_spec), out_specs=(row_spec, cache_spec, cache_spec), check_vma=False)
```
